32 devices in a mesh: lon: 16 (over z, y, x), lat: 2 (over core).
Axes of the slice: x: 2, y: 2, z: 4, core: 2. Of those that a mesh axis runs over, the one named last changes fastest.
Arguments:
- u_vel: float32 [40, 128, 1024], P(None, 'lon', 'lat'), may hold values from -6 to 6
- v_vel: float32 [40, 128, 1024], P(None, 'lon', 'lat'), may hold values from -6 to 6
- thickness: float32 [40], replicated, may hold values from 0.5 to 2
- depth: float32 [128, 1024], P('lon', 'lat'), may hold values from 0.5 to 2
- sea_mask: int32 [128, 1024], P('lon', 'lat'), may hold values 0 or 1
- damping: float32 [128, 1024], P('lon', 'lat'), may hold values from 0.1 to 2
- eta_prev: float32 [128, 1024], P('lon', 'lat'), may hold values from -6 to 6
Outputs:
- surface: float32 [128, 1024], P('lon', 'lat')
- residual: float32 [128, 1024], P('lon', 'lat')
The draws below stay inside these ranges and needn't reach their ends.
All inputs are finite; a program needn't handle non-finite values. No bound on the sum of `sea_mask` on one device may be relied on, other than what follows from the above.
Results may differ from the reference program's by a relative error of at most 0.0003.
Values sent between devices are 32-bit elements; how exact they have to be, the bound alone decides.
A program may use at most 64 MiB of HBM per device.

```python
import math
import jax
import jax.numpy as jnp
from jax import lax

LEVELS = 40
ITERS = 3
NX = 128
NY = 1024


def place_ends(values, stream_key, smallest, high):
    longest = values.shape.index(max(values.shape))
    spots = []
    for shift in (0, 1):
        where = [jax.random.randint(jax.random.fold_in(stream_key, axis), (), 0, length) for axis, length in enumerate(values.shape)]
        where[longest] = (where[longest] + shift) % values.shape[longest]
        spots.append(tuple(where))
    return values.at[spots[0]].set(smallest).at[spots[1]].set(high)


def shard_levels(key, shape, split, smallest, high):
    def one(position, parts):
        steps = jax.random.uniform(jax.random.fold_in(jax.random.fold_in(key, 6), position), (parts,), jnp.float32, smallest / len(split), high / len(split))
        return jnp.repeat(jnp.exp(steps), shape[position] // parts).reshape((-1,) + (1,) * (len(shape) - position - 1))

    loudness = one(*split[0])
    for cut in split[1:]:
        loudness = loudness * one(*cut)
    return loudness


def centred(stream_key, dims, scale, reach, split=(), dtype=jnp.bfloat16):
    values = jax.random.normal(stream_key, dims, jnp.float32) * scale
    if len(split) > 0:
        values = shard_levels(stream_key, dims, split, -0.22, 0.18) * values
    return jnp.clip(values, min=-reach, max=reach).astype(dtype)


def setup_inputs(seed: int = 0) -> dict:
    seeds = jax.random.split(jax.random.key(seed), 8)
    return {
        "u_vel": centred(seeds[0], (LEVELS, NX, NY), 1.0, 6.0, ((1, 16), (2, 2)), jnp.float32),
        "v_vel": centred(seeds[1], (LEVELS, NX, NY), 1.0, 6.0, ((1, 16), (2, 2)), jnp.float32),
        "thickness": jnp.clip(jnp.exp(jax.random.uniform(seeds[2], (LEVELS,), jnp.float32, math.log(0.5), math.log(2.0))), 0.5, 2.0),
        "depth": jnp.clip(jnp.exp(math.log(2.0) - 1.3862944 * jax.random.uniform(seeds[3], (NX, NY), jnp.float32) ** shard_levels(seeds[3], (NX, NY), ((0, 16), (1, 2)), -0.2, 0.2)), 0.5, 2.0),
        "sea_mask": place_ends((jax.random.randint(seeds[4], (NX, NY), 0, 8) < 7).astype(jnp.int32), jax.random.fold_in(seeds[4], 1), 0, 1),
        "damping": jnp.clip(jnp.exp(math.log(2.0) - 2.9957323 * jax.random.uniform(seeds[5], (NX, NY), jnp.float32) ** shard_levels(seeds[5], (NX, NY), ((0, 16), (1, 2)), -0.2, 0.2)), 0.1, 2.0),
        "eta_prev": centred(seeds[6], (NX, NY), 1.0, 6.0, ((0, 16), (1, 2)), jnp.float32),
    }


def faces(depth, wet):
    north_ok = (lax.broadcasted_iota(jnp.int32, wet.shape, 1) < wet.shape[1] - 1).astype(jnp.float32)
    wet_east = wet * jnp.roll(wet, -1, 0)
    wet_north = wet * jnp.roll(wet, -1, 1) * north_ok
    face_x = wet_east * 0.5 * (depth + jnp.roll(depth, -1, 0))
    face_y = wet_north * 0.5 * (depth + jnp.roll(depth, -1, 1))
    return (wet_east, wet_north, face_x, face_y)

def operate(field, diag, face_x, face_y):
    result = diag * field - face_x * jnp.roll(field, -1, 0) - jnp.roll(face_x, 1, 0) * jnp.roll(field, 1, 0)
    return result - face_y * jnp.roll(field, -1, 1) - jnp.roll(face_y, 1, 1) * jnp.roll(field, 1, 1)

def reference(u_vel, v_vel, thickness, depth, sea_mask, damping, eta_prev):
    wet = sea_mask.astype(jnp.float32)
    wet_east, wet_north, face_x, face_y = faces(depth, wet)
    scale = 1.0 / math.sqrt(LEVELS)
    east_flux = wet_east * jnp.einsum('k,kxy->xy', thickness, u_vel, precision=lax.Precision.HIGHEST) * scale
    north_flux = wet_north * jnp.einsum('k,kxy->xy', thickness, v_vel, precision=lax.Precision.HIGHEST) * scale
    diverge = east_flux - jnp.roll(east_flux, 1, 0) + north_flux - jnp.roll(north_flux, 1, 1)
    rhs = wet * (damping * eta_prev - diverge)
    diag = damping + face_x + jnp.roll(face_x, 1, 0) + face_y + jnp.roll(face_y, 1, 1)
    surface = jnp.zeros_like(rhs)
    residual = rhs
    precond = residual / diag
    image = operate(precond, diag, face_x, face_y)
    gamma_now = jnp.sum(residual * precond)
    delta_now = jnp.sum(image * precond)
    step_size = gamma_now / delta_now
    direction, along_dir = (precond, image)
    for sweep in range(ITERS):
        surface = surface + step_size * direction
        residual = residual - step_size * along_dir
        if sweep + 1 < ITERS:
            precond = residual / diag
            image = operate(precond, diag, face_x, face_y)
            gamma_next = jnp.sum(residual * precond)
            delta_now = jnp.sum(image * precond)
            ratio_next = gamma_next / gamma_now
            step_size = gamma_next / (delta_now - ratio_next * gamma_next / step_size)
            direction = precond + ratio_next * direction
            along_dir = image + ratio_next * along_dir
            gamma_now = gamma_next
    return (surface, residual)
```

```python
import functools
import math

import jax
import jax.numpy as jnp
from jax import lax
from jax.experimental import pallas as pl
from jax.experimental.pallas import tpu as pltpu
from jax.sharding import PartitionSpec as P

MESH = pl.DeviceIdType.MESH
HALO = 4
FIELDS = 5
LANES = 128
ROWS = 8


def scalars(nu):
    def form(c, shift):
        total = None
        for i, ci in enumerate(c):
            for j, cj in enumerate(c):
                if j < i:
                    continue
                term = ci * cj * nu[i + j + shift]
                term = term if i == j else term + term
                total = term if total is None else total + term
        return total

    def apply(c):
        out = list(c) + [None]
        for k, ck in enumerate(c):
            out[k + 1] = -ck if out[k + 1] is None else out[k + 1] - ck
        return out

    def axpy(a, x, y):
        out = []
        for k in range(max(len(x), len(y))):
            if k >= len(x):
                out.append(y[k])
            elif k >= len(y):
                out.append(a * x[k])
            else:
                out.append(y[k] + a * x[k])
        return out

    one = jnp.ones_like(nu[0])
    residual = [one]
    direction = [one]
    gamma = nu[0]
    step = gamma / (nu[0] - nu[1])
    surface = [step]
    residual = axpy(-step, apply(direction), residual)
    for _ in range(2):
        gamma_next = form(residual, 0)
        delta = gamma_next - form(residual, 1)
        ratio = gamma_next / gamma
        step = gamma_next / (delta - ratio * gamma_next / step)
        direction = axpy(ratio, direction, residual)
        surface = axpy(step, direction, surface)
        residual = axpy(-step, apply(direction), residual)
        gamma = gamma_next
    return surface, residual


def kernel(
    lon_n, lat_n, lon_axis, lat_axis,
    thick, u_hbm, v_hbm, depth_hbm, mask_hbm, damp_hbm, eta_hbm,
    surface_out, residual_out,
    u_buf, v_buf, depth_v, mask_v, damp_v, eta_v,
    send_lon, recv_lon, send_lat, recv_lat, recv_diag, row_send, row_recv,
    load_sem, halo_send, halo_recv, all_send, all_recv,
):
    levels, rows, cols = u_hbm.shape
    n = lon_n * lat_n
    lon = lax.axis_index(lon_axis)
    lat = lax.axis_index(lat_axis)
    me = lon * lat_n + lat

    def peer(k):
        flat = lax.rem(me + k, n)
        return (flat // lat_n, lax.rem(flat, lat_n))

    def each_peer(f):
        if n <= 64:
            for k in range(1, n):
                f(k)
        else:
            lax.fori_loop(1, n, lambda k, c: (f(k), c)[1], 0)

    loads = []
    for k, (src, dst) in enumerate((
        (u_hbm, u_buf), (v_hbm, v_buf), (depth_hbm, depth_v), (mask_hbm, mask_v), (damp_hbm, damp_v), (eta_hbm, eta_v)
    )):
        copy = pltpu.make_async_copy(src, dst, load_sem.at[k])
        copy.start()
        loads.append(copy)

    barrier = pltpu.get_barrier_semaphore()
    each_peer(lambda k: pl.semaphore_signal(barrier, inc=1, device_id=peer(k), device_id_type=MESH))

    for copy in loads[2:]:
        copy.wait()
    wet_own = mask_v[...].astype(jnp.float32)
    damp_own = damp_v[...]
    own = [depth_v[...] * wet_own, damp_own, damp_own * eta_v[...]]
    scale = 1.0 / math.sqrt(levels)
    for copy, buf in ((loads[0], u_buf), (loads[1], v_buf)):
        copy.wait()
        total = [None] * 4
        for k in range(levels):
            term = thick[k] * buf[k]
            total[k % 4] = term if total[k % 4] is None else total[k % 4] + term
        own.append(((total[0] + total[1]) + (total[2] + total[3])) * scale)

    for f in range(FIELDS):
        send_lon[0, f] = own[f][:HALO]
        send_lon[1, f] = own[f][rows - HALO:]
        send_lat[0, f] = own[f][:, :LANES]
        send_lat[1, f] = own[f][:, cols - LANES:]

    pl.semaphore_wait(barrier, n - 1)

    west = lax.rem(lon + lon_n - 1, lon_n)
    east = lax.rem(lon + 1, lon_n)

    def remote(src, dst, sem, target):
        return pltpu.make_async_remote_copy(
            src_ref=src, dst_ref=dst, send_sem=halo_send.at[sem], recv_sem=halo_recv.at[sem],
            device_id=target, device_id_type=MESH,
        )

    lon_copies = [remote(send_lon.at[h], recv_lon.at[h], h, (west if h == 0 else east, lat)) for h in (0, 1)]
    lat_copies = []
    for part in (0, 1):
        other = lat - 1 if part == 0 else lat + 1
        piece = pl.ds(0, LANES) if part == 0 else pl.ds(cols - LANES, LANES)
        group = [remote(send_lat.at[part], recv_lat.at[part], 2 + part, (lon, other))]
        for h in (0, 1):
            group.append(remote(
                send_lon.at[h, :, :, piece], recv_diag.at[h, part], 4 + 2 * part + h, (west if h == 0 else east, other)
            ))
        lat_copies.append(group)
    has_south = lat > 0
    has_north = lat < lat_n - 1
    sends = (has_south, has_north)
    gets = (has_north, has_south)

    for copy in lon_copies:
        copy.start()
    for part in (0, 1):
        @pl.when(sends[part])
        def _():
            for copy in lat_copies[part][1:]:
                copy.start()
            lat_copies[part][0].start()

        @pl.when(jnp.logical_not(gets[part]))
        def _():
            recv_lat[part] = jnp.zeros((FIELDS, rows, LANES), jnp.float32)
            recv_diag[0, part] = jnp.zeros((FIELDS, HALO, LANES), jnp.float32)
            recv_diag[1, part] = jnp.zeros((FIELDS, HALO, LANES), jnp.float32)

    for part in (0, 1):
        @pl.when(gets[part])
        def _():
            for copy in lat_copies[part]:
                copy.wait_recv()
    for copy in lon_copies:
        copy.wait_recv()

    lane = lax.broadcasted_iota(jnp.int32, (rows, LANES), 1)
    north_side = lane < LANES // 2

    def extended(f):
        sides = jnp.where(north_side, recv_lat[0, f], recv_lat[1, f])
        over = jnp.concatenate([recv_lon[0, f], recv_lon[1, f]], axis=0)
        corner_north = jnp.concatenate([recv_diag[0, 0, f], recv_diag[1, 0, f]], axis=0)
        corner_south = jnp.concatenate([recv_diag[0, 1, f], recv_diag[1, 1, f]], axis=0)
        corner = jnp.where(north_side, corner_north, corner_south)
        return jnp.concatenate(
            [jnp.concatenate([own[f], sides], axis=1), jnp.concatenate([over, corner], axis=1)], axis=0
        )

    high, wide = 2 * rows, cols + LANES

    def up(x, axis):
        return pltpu.roll(x, x.shape[axis] - 1, axis)

    def down(x, axis):
        return pltpu.roll(x, 1, axis)

    deep, damp, forced, sum_east, sum_north = [extended(f) for f in range(FIELDS)]
    wet = (deep > 0.0).astype(jnp.float32)
    damp = jnp.where(damp > 0.0, damp, 1.0)
    wet_x = wet * up(wet, 0)
    wet_y = wet * up(wet, 1)
    face_x = wet_x * 0.5 * (deep + up(deep, 0))
    face_y = wet_y * 0.5 * (deep + up(deep, 1))
    flux_x = wet_x * sum_east
    flux_y = wet_y * sum_north
    rhs = wet * (forced - (flux_x - down(flux_x, 0) + flux_y - down(flux_y, 1)))
    face_w, face_s = down(face_x, 0), down(face_y, 1)
    inverse = 1.0 / (damp + face_x + face_w + face_y + face_s)

    def off(p):
        return face_x * up(p, 0) + face_w * down(p, 0) + face_y * up(p, 1) + face_s * down(p, 1)

    p0 = rhs * inverse
    w1 = off(p0)
    p1 = w1 * inverse
    w2 = off(p1)
    p2 = w2 * inverse
    w3 = off(p2)
    w0, w1, w2, w3, p0, p1, p2 = [x[:rows, :cols] for x in (rhs, w1, w2, w3, p0, p1, p2)]

    lines = []
    for a, b in ((w0, p0), (w0, p1), (w1, p1), (w1, p2), (w2, p2), (w3, p2)):
        product = a * b
        folded = product[:, :LANES]
        for c in range(LANES, cols, LANES):
            folded = folded + product[:, c:c + LANES]
        lines.append(jnp.sum(folded, axis=0, keepdims=True))
    zero = jnp.zeros_like(lines[0])
    table = jnp.concatenate(lines + [zero] * (8 - len(lines)), axis=0)
    table = jnp.broadcast_to(jnp.sum(table, axis=1, keepdims=True), (8, LANES))
    pick = lax.broadcasted_iota(jnp.int32, (8, LANES), 1) == lax.broadcasted_iota(jnp.int32, (8, LANES), 0)
    row = jnp.sum(jnp.where(pick, table, 0.0), axis=0, keepdims=True)
    row_send[...] = row
    row_recv[me] = row

    def send_row(k):
        pltpu.make_async_remote_copy(
            src_ref=row_send, dst_ref=row_recv.at[me], send_sem=all_send, recv_sem=all_recv,
            device_id=peer(k), device_id_type=MESH,
        ).start()

    each_peer(send_row)

    for copy in lon_copies:
        copy.wait_send()
    for part in (0, 1):
        @pl.when(sends[part])
        def _():
            for copy in lat_copies[part]:
                copy.wait_send()

    others = row_recv.at[pl.ds(0, n - 1)]
    pltpu.make_async_copy(others, others, all_recv).wait()
    total = jnp.sum(row_recv[...], axis=0)
    nu = [jnp.broadcast_to(total[:, k:k + 1], (ROWS, LANES)) for k in range(6)]
    s, r = scalars(nu)
    for c in range(0, cols, LANES):
        part = slice(c, c + LANES)
        surface_out[:, part] = s[0] * p0[:, part] + s[1] * p1[:, part] + s[2] * p2[:, part]
        residual_out[:, part] = (r[0] * w0[:, part] + r[1] * w1[:, part]) + (r[2] * w2[:, part] + r[3] * w3[:, part])
    pltpu.make_async_copy(others, others, all_send).wait()


def solution(mesh):
    lon_n, lat_n = mesh.shape["lon"], mesh.shape["lat"]
    n = lon_n * lat_n

    def body(u_vel, v_vel, thickness, depth, sea_mask, damping, eta_prev):
        levels, rows, cols = u_vel.shape
        f32 = jnp.float32
        hbm = pl.BlockSpec(memory_space=pl.ANY)
        vmem = pl.BlockSpec(memory_space=pltpu.VMEM)
        shape = jax.ShapeDtypeStruct((rows, cols), f32)
        return pl.pallas_call(
            functools.partial(kernel, lon_n, lat_n, "lon", "lat"),
            out_shape=(shape, shape),
            in_specs=[pl.BlockSpec(memory_space=pltpu.SMEM)] + [hbm] * 6,
            out_specs=(vmem, vmem),
            scratch_shapes=[
                pltpu.VMEM((levels, rows, cols), f32),
                pltpu.VMEM((levels, rows, cols), f32),
                pltpu.VMEM((rows, cols), f32),
                pltpu.VMEM((rows, cols), jnp.int32),
                pltpu.VMEM((rows, cols), f32),
                pltpu.VMEM((rows, cols), f32),
                pltpu.VMEM((2, FIELDS, HALO, cols), f32),
                pltpu.VMEM((2, FIELDS, HALO, cols), f32),
                pltpu.VMEM((2, FIELDS, rows, LANES), f32),
                pltpu.VMEM((2, FIELDS, rows, LANES), f32),
                pltpu.VMEM((2, 2, FIELDS, HALO, LANES), f32),
                pltpu.VMEM((1, LANES), f32),
                pltpu.VMEM((n, 1, LANES), f32),
                pltpu.SemaphoreType.DMA((6,)),
                pltpu.SemaphoreType.DMA((8,)),
                pltpu.SemaphoreType.DMA((8,)),
                pltpu.SemaphoreType.DMA,
                pltpu.SemaphoreType.DMA,
            ],
            compiler_params=pltpu.CompilerParams(collective_id=0, has_side_effects=True),
        )(thickness, u_vel, v_vel, depth, sea_mask, damping, eta_prev)

    placed = P("lon", "lat")
    return jax.shard_map(
        body,
        mesh=mesh,
        in_specs=(P(None, "lon", "lat"), P(None, "lon", "lat"), P(), placed, placed, placed, placed),
        out_specs=(placed, placed),
        check_vma=False,
    )
```

```python
import functools
import math

import jax
import jax.numpy as jnp
from jax import lax
from jax.experimental import pallas as pl
from jax.experimental.pallas import tpu as pltpu
from jax.sharding import PartitionSpec as P

MESH = pl.DeviceIdType.MESH
HALO = 4
FIELDS = 5
LANES = 128
ROWS = 8


def scalars(nu):
    def form(c, shift):
        total = None
        for i, ci in enumerate(c):
            for j, cj in enumerate(c):
                if j < i:
                    continue
                term = ci * cj * nu[i + j + shift]
                term = term if i == j else term + term
                total = term if total is None else total + term
        return total

    def apply(c):
        out = list(c) + [None]
        for k, ck in enumerate(c):
            out[k + 1] = -ck if out[k + 1] is None else out[k + 1] - ck
        return out

    def axpy(a, x, y):
        out = []
        for k in range(max(len(x), len(y))):
            if k >= len(x):
                out.append(y[k])
            elif k >= len(y):
                out.append(a * x[k])
            else:
                out.append(y[k] + a * x[k])
        return out

    one = jnp.ones_like(nu[0])
    residual = [one]
    direction = [one]
    gamma = nu[0]
    step = gamma / (nu[0] - nu[1])
    surface = [step]
    residual = axpy(-step, apply(direction), residual)
    for _ in range(2):
        gamma_next = form(residual, 0)
        delta = gamma_next - form(residual, 1)
        ratio = gamma_next / gamma
        step = gamma_next / (delta - ratio * gamma_next / step)
        direction = axpy(ratio, direction, residual)
        surface = axpy(step, direction, surface)
        residual = axpy(-step, apply(direction), residual)
        gamma = gamma_next
    return surface, residual


def kernel(
    lon_n, lat_n, lon_axis, lat_axis,
    thick_hbm, u_hbm, v_hbm, depth_hbm, mask_hbm, damp_hbm, eta_hbm,
    surface_out, residual_out,
    thick, u_buf, v_buf, depth_v, mask_v, damp_v, eta_v,
    send_lon, recv_lon, send_lat, recv_lat, recv_diag, row_send, row_recv,
    load_sem, halo_send, halo_recv, all_send, all_recv,
):
    levels, rows, cols = u_hbm.shape
    n = lon_n * lat_n
    lon = lax.axis_index(lon_axis)
    lat = lax.axis_index(lat_axis)
    me = lon * lat_n + lat

    def peer(k):
        flat = lax.rem(me + k, n)
        return (flat // lat_n, lax.rem(flat, lat_n))

    def each_peer(f):
        if n <= 64:
            for k in sorted(range(1, n), key=lambda k: -min(k, n - k)):
                f(k)
        else:
            lax.fori_loop(1, n, lambda k, c: (f(k), c)[1], 0)

    loads = []
    for k, (src, dst) in enumerate((
        (u_hbm, u_buf), (v_hbm, v_buf), (depth_hbm, depth_v), (mask_hbm, mask_v), (damp_hbm, damp_v), (eta_hbm, eta_v),
        (thick_hbm, thick)
    )):
        copy = pltpu.make_async_copy(src, dst, load_sem.at[k])
        copy.start()
        loads.append(copy)

    barrier = pltpu.get_barrier_semaphore()
    each_peer(lambda k: pl.semaphore_signal(barrier, inc=1, device_id=peer(k), device_id_type=MESH))

    for copy in loads[2:]:
        copy.wait()
    wet_own = mask_v[...].astype(jnp.float32)
    damp_own = damp_v[...]
    own = [depth_v[...] * wet_own, damp_own, damp_own * eta_v[...]]
    scale = 1.0 / math.sqrt(levels)
    for copy, buf in ((loads[0], u_buf), (loads[1], v_buf)):
        copy.wait()
        total = [None] * 4
        for k in range(levels):
            term = thick[k] * buf[k]
            total[k % 4] = term if total[k % 4] is None else total[k % 4] + term
        own.append(((total[0] + total[1]) + (total[2] + total[3])) * scale)

    for f in range(FIELDS):
        send_lon[0, f] = own[f][:HALO]
        send_lon[1, f] = own[f][rows - HALO:]
        send_lat[0, f] = own[f][:, :LANES]
        send_lat[1, f] = own[f][:, cols - LANES:]

    pl.semaphore_wait(barrier, n - 1)

    west = lax.rem(lon + lon_n - 1, lon_n)
    east = lax.rem(lon + 1, lon_n)

    def remote(src, dst, sem, target):
        return pltpu.make_async_remote_copy(
            src_ref=src, dst_ref=dst, send_sem=halo_send.at[sem], recv_sem=halo_recv.at[sem],
            device_id=target, device_id_type=MESH,
        )

    lon_copies = [remote(send_lon.at[h], recv_lon.at[h], h, (west if h == 0 else east, lat)) for h in (0, 1)]
    lat_copies = []
    for part in (0, 1):
        other = lat - 1 if part == 0 else lat + 1
        piece = pl.ds(0, LANES) if part == 0 else pl.ds(cols - LANES, LANES)
        group = [remote(send_lat.at[part], recv_lat.at[part], 2 + part, (lon, other))]
        for h in (0, 1):
            group.append(remote(
                send_lon.at[h, :, :, piece], recv_diag.at[h, part], 4 + 2 * part + h, (west if h == 0 else east, other)
            ))
        lat_copies.append(group)
    has_south = lat > 0
    has_north = lat < lat_n - 1
    sends = (has_south, has_north)
    gets = (has_north, has_south)

    for copy in lon_copies:
        copy.start()
    for part in (0, 1):
        @pl.when(sends[part])
        def _():
            for copy in lat_copies[part][1:]:
                copy.start()
            lat_copies[part][0].start()

        @pl.when(jnp.logical_not(gets[part]))
        def _():
            recv_lat[part] = jnp.zeros((FIELDS, rows, LANES), jnp.float32)
            recv_diag[0, part] = jnp.zeros((FIELDS, HALO, LANES), jnp.float32)
            recv_diag[1, part] = jnp.zeros((FIELDS, HALO, LANES), jnp.float32)

    for part in (0, 1):
        @pl.when(gets[part])
        def _():
            for copy in lat_copies[part]:
                copy.wait_recv()
    for copy in lon_copies:
        copy.wait_recv()

    lane = lax.broadcasted_iota(jnp.int32, (rows, LANES), 1)
    north_side = lane < LANES // 2

    def extended(f):
        sides = jnp.where(north_side, recv_lat[0, f], recv_lat[1, f])
        over = jnp.concatenate([recv_lon[0, f], recv_lon[1, f]], axis=0)
        corner_north = jnp.concatenate([recv_diag[0, 0, f], recv_diag[1, 0, f]], axis=0)
        corner_south = jnp.concatenate([recv_diag[0, 1, f], recv_diag[1, 1, f]], axis=0)
        corner = jnp.where(north_side, corner_north, corner_south)
        return jnp.concatenate(
            [jnp.concatenate([own[f], sides], axis=1), jnp.concatenate([over, corner], axis=1)], axis=0
        )

    high, wide = 2 * rows, cols + LANES

    def up(x, axis):
        return pltpu.roll(x, x.shape[axis] - 1, axis)

    def down(x, axis):
        return pltpu.roll(x, 1, axis)

    deep, damp, forced, sum_east, sum_north = [extended(f) for f in range(FIELDS)]
    wet = (deep > 0.0).astype(jnp.float32)
    damp = jnp.where(damp > 0.0, damp, 1.0)
    wet_x = wet * up(wet, 0)
    wet_y = wet * up(wet, 1)
    face_x = wet_x * 0.5 * (deep + up(deep, 0))
    face_y = wet_y * 0.5 * (deep + up(deep, 1))
    flux_x = wet_x * sum_east
    flux_y = wet_y * sum_north
    rhs = wet * (forced - (flux_x - down(flux_x, 0) + flux_y - down(flux_y, 1)))
    face_w, face_s = down(face_x, 0), down(face_y, 1)
    inverse = 1.0 / (damp + face_x + face_w + face_y + face_s)

    def off(p):
        return face_x * up(p, 0) + face_w * down(p, 0) + face_y * up(p, 1) + face_s * down(p, 1)

    p0 = rhs * inverse
    w1 = off(p0)
    p1 = w1 * inverse
    w2 = off(p1)
    p2 = w2 * inverse
    w3 = off(p2)
    w0, w1, w2, w3, p0, p1, p2 = [x[:rows, :cols] for x in (rhs, w1, w2, w3, p0, p1, p2)]

    lines = []
    for a, b in ((w0, p0), (w0, p1), (w1, p1), (w1, p2), (w2, p2), (w3, p2)):
        product = a * b
        folded = product[:, :LANES]
        for c in range(LANES, cols, LANES):
            folded = folded + product[:, c:c + LANES]
        lines.append(jnp.sum(folded, axis=0, keepdims=True))
    zero = jnp.zeros_like(lines[0])
    table = jnp.concatenate(lines + [zero] * (8 - len(lines)), axis=0)
    table = jnp.broadcast_to(jnp.sum(table, axis=1, keepdims=True), (8, LANES))
    pick = lax.broadcasted_iota(jnp.int32, (8, LANES), 1) == lax.broadcasted_iota(jnp.int32, (8, LANES), 0)
    row = jnp.sum(jnp.where(pick, table, 0.0), axis=0, keepdims=True)
    row_send[...] = row
    row_recv[me] = row

    def send_row(k):
        pltpu.make_async_remote_copy(
            src_ref=row_send, dst_ref=row_recv.at[me], send_sem=all_send, recv_sem=all_recv,
            device_id=peer(k), device_id_type=MESH,
        ).start()

    each_peer(send_row)

    for copy in lon_copies:
        copy.wait_send()
    for part in (0, 1):
        @pl.when(sends[part])
        def _():
            for copy in lat_copies[part]:
                copy.wait_send()

    others = row_recv.at[pl.ds(0, n - 1)]
    pltpu.make_async_copy(others, others, all_recv).wait()
    total = jnp.sum(row_recv[...], axis=0)
    nu = [jnp.broadcast_to(total[:, k:k + 1], (ROWS, LANES)) for k in range(6)]
    s, r = scalars(nu)
    for c in range(0, cols, LANES):
        part = slice(c, c + LANES)
        surface_out[:, part] = s[0] * p0[:, part] + s[1] * p1[:, part] + s[2] * p2[:, part]
        residual_out[:, part] = (r[0] * w0[:, part] + r[1] * w1[:, part]) + (r[2] * w2[:, part] + r[3] * w3[:, part])
    pltpu.make_async_copy(others, others, all_send).wait()


def solution(mesh):
    lon_n, lat_n = mesh.shape["lon"], mesh.shape["lat"]
    n = lon_n * lat_n

    def body(u_vel, v_vel, thickness, depth, sea_mask, damping, eta_prev):
        levels, rows, cols = u_vel.shape
        f32 = jnp.float32
        hbm = pl.BlockSpec(memory_space=pl.ANY)
        vmem = pl.BlockSpec(memory_space=pltpu.VMEM)
        shape = pltpu.VMEM((rows, cols), f32)
        return pl.pallas_call(
            functools.partial(kernel, lon_n, lat_n, "lon", "lat"),
            out_shape=(shape, shape),
            in_specs=[hbm] * 7,
            out_specs=(vmem, vmem),
            scratch_shapes=[
                pltpu.SMEM((levels,), f32),
                pltpu.VMEM((levels, rows, cols), f32),
                pltpu.VMEM((levels, rows, cols), f32),
                pltpu.VMEM((rows, cols), f32),
                pltpu.VMEM((rows, cols), jnp.int32),
                pltpu.VMEM((rows, cols), f32),
                pltpu.VMEM((rows, cols), f32),
                pltpu.VMEM((2, FIELDS, HALO, cols), f32),
                pltpu.VMEM((2, FIELDS, HALO, cols), f32),
                pltpu.VMEM((2, FIELDS, rows, LANES), f32),
                pltpu.VMEM((2, FIELDS, rows, LANES), f32),
                pltpu.VMEM((2, 2, FIELDS, HALO, LANES), f32),
                pltpu.VMEM((1, LANES), f32),
                pltpu.VMEM((n, 1, LANES), f32),
                pltpu.SemaphoreType.DMA((7,)),
                pltpu.SemaphoreType.DMA((8,)),
                pltpu.SemaphoreType.DMA((8,)),
                pltpu.SemaphoreType.DMA,
                pltpu.SemaphoreType.DMA,
            ],
            compiler_params=pltpu.CompilerParams(collective_id=0, has_side_effects=True),
        )(thickness, u_vel, v_vel, depth, sea_mask, damping, eta_prev)

    placed = P("lon", "lat")
    return jax.shard_map(
        body,
        mesh=mesh,
        in_specs=(P(None, "lon", "lat"), P(None, "lon", "lat"), P(), placed, placed, placed, placed),
        out_specs=(placed, placed),
        check_vma=False,
    )
```

```python
import functools
import math

import jax
import jax.numpy as jnp
from jax import lax
from jax.experimental import pallas as pl
from jax.experimental.pallas import tpu as pltpu
from jax.sharding import PartitionSpec as P

MESH = pl.DeviceIdType.MESH
HALO = 4
FIELDS = 5
LANES = 128
ROWS = 8


def scalars(nu):
    def form(c, shift):
        total = None
        for i, ci in enumerate(c):
            for j, cj in enumerate(c):
                if j < i:
                    continue
                term = ci * cj * nu[i + j + shift]
                term = term if i == j else term + term
                total = term if total is None else total + term
        return total

    def apply(c):
        out = list(c) + [None]
        for k, ck in enumerate(c):
            out[k + 1] = -ck if out[k + 1] is None else out[k + 1] - ck
        return out

    def axpy(a, x, y):
        out = []
        for k in range(max(len(x), len(y))):
            if k >= len(x):
                out.append(y[k])
            elif k >= len(y):
                out.append(a * x[k])
            else:
                out.append(y[k] + a * x[k])
        return out

    one = jnp.ones_like(nu[0])
    residual = [one]
    direction = [one]
    gamma = nu[0]
    step = gamma / (nu[0] - nu[1])
    surface = [step]
    residual = axpy(-step, apply(direction), residual)
    for _ in range(2):
        gamma_next = form(residual, 0)
        delta = gamma_next - form(residual, 1)
        ratio = gamma_next / gamma
        step = gamma_next / (delta - ratio * gamma_next / step)
        direction = axpy(ratio, direction, residual)
        surface = axpy(step, direction, surface)
        residual = axpy(-step, apply(direction), residual)
        gamma = gamma_next
    return surface, residual


def kernel(
    lon_n, lat_n, lon_axis, lat_axis,
    thick_hbm, u_hbm, v_hbm, depth_hbm, mask_hbm, damp_hbm, eta_hbm,
    surface_out, residual_out,
    thick, u_buf, v_buf, depth_v, mask_v, damp_v, eta_v,
    send_lon, recv_lon, send_lat, recv_lat, send_diag, recv_diag, row_send, row_recv,
    load_sem, halo_send, halo_recv, all_send, all_recv,
):
    levels, rows, cols = u_hbm.shape
    n = lon_n * lat_n
    lon = lax.axis_index(lon_axis)
    lat = lax.axis_index(lat_axis)
    me = lon * lat_n + lat

    def peer(k):
        flat = lax.rem(me + k, n)
        return (flat // lat_n, lax.rem(flat, lat_n))

    def each_peer(f):
        if n <= 64:
            for k in sorted(range(1, n), key=lambda k: -min(k, n - k)):
                f(k)
        else:
            lax.fori_loop(1, n, lambda k, c: (f(k), c)[1], 0)

    loads = []
    for k, (src, dst) in enumerate((
        (u_hbm, u_buf), (v_hbm, v_buf), (depth_hbm, depth_v), (mask_hbm, mask_v), (damp_hbm, damp_v), (eta_hbm, eta_v),
        (thick_hbm, thick)
    )):
        copy = pltpu.make_async_copy(src, dst, load_sem.at[k])
        copy.start()
        loads.append(copy)

    barrier = pltpu.get_barrier_semaphore()
    each_peer(lambda k: pl.semaphore_signal(barrier, inc=1, device_id=peer(k), device_id_type=MESH))

    def up(x, axis):
        return pltpu.roll(x, x.shape[axis] - 1, axis)

    def down(x, axis):
        return pltpu.roll(x, 1, axis)

    for copy in loads[2:]:
        copy.wait()
    wet_own = mask_v[...].astype(jnp.float32)
    damp_own = damp_v[...]
    deep_own = depth_v[...] * wet_own
    forced_own = wet_own * (damp_own * eta_v[...])
    row_own = lax.broadcasted_iota(jnp.int32, (rows, cols), 0)
    col_own = lax.broadcasted_iota(jnp.int32, (rows, cols), 1)
    inner_x = jnp.where(row_own < rows - 1, wet_own * up(wet_own, 0), 0.0)
    inner_y = jnp.where(col_own < cols - 1, wet_own * up(wet_own, 1), 0.0)
    scale = 1.0 / math.sqrt(levels)
    column = []
    for copy, buf in ((loads[0], u_buf), (loads[1], v_buf)):
        copy.wait()
        total = [None] * 4
        for k in range(levels):
            term = thick[k] * buf[k]
            total[k % 4] = term if total[k % 4] is None else total[k % 4] + term
        column.append(((total[0] + total[1]) + (total[2] + total[3])) * scale)
    east_own, north_own = column
    inner_x = inner_x * east_own
    inner_y = inner_y * north_own
    part_own = forced_own - (inner_x - down(inner_x, 0) + inner_y - down(inner_y, 1))
    last_east = jnp.broadcast_to(east_own[rows - 1:], (rows, cols))
    part_sent = jnp.where(row_own == rows - HALO, last_east, part_own)
    own = [deep_own, damp_own, part_own, east_own, north_own]
    tiles = cols // LANES
    lane_short = lax.broadcasted_iota(jnp.int32, (rows, LANES), 1)
    for f, x in enumerate((deep_own, damp_own, part_sent)):
        for c in range(tiles):
            piece = x[:, c * LANES:(c + 1) * LANES]
            send_lon[0, f * tiles + c] = piece[:HALO]
            send_lon[1, f * tiles + c] = piece[rows - HALO:]
    north_last = north_own[:, cols - LANES:]
    send_lon[0, 3 * tiles] = north_last[:HALO]
    send_lon[1, 3 * tiles] = north_last[rows - HALO:]
    for part in (0, 1):
        packed = None
        for f, x in enumerate((deep_own, damp_own, part_sent, north_own)):
            edge = x[:, :LANES] if part == 0 else x[:, cols - LANES:]
            edge = edge if f == 0 else pltpu.roll(edge, HALO * f if part == 0 else LANES - HALO * f, 1)
            away = lane_short if part == 0 else LANES - 1 - lane_short
            packed = edge if packed is None else jnp.where(away >= HALO * f, edge, packed)
        send_diag[0, part] = packed[:HALO]
        send_diag[1, part] = packed[rows - HALO:]
    for f in range(FIELDS):
        send_lat[0, f] = own[f][:, :LANES]
        send_lat[1, f] = own[f][:, cols - LANES:]

    pl.semaphore_wait(barrier, n - 1)

    west = lax.rem(lon + lon_n - 1, lon_n)
    east = lax.rem(lon + 1, lon_n)

    def remote(src, dst, sem, target):
        return pltpu.make_async_remote_copy(
            src_ref=src, dst_ref=dst, send_sem=halo_send.at[sem], recv_sem=halo_recv.at[sem],
            device_id=target, device_id_type=MESH,
        )

    lon_copies = [remote(send_lon.at[h], recv_lon.at[h], h, (west if h == 0 else east, lat)) for h in (0, 1)]
    lat_copies = []
    for part in (0, 1):
        other = lat - 1 if part == 0 else lat + 1
        group = [remote(send_lat.at[part], recv_lat.at[part], 2 + part, (lon, other))]
        for h in (0, 1):
            group.append(remote(
                send_diag.at[h, part], recv_diag.at[h, part], 4 + 2 * part + h, (west if h == 0 else east, other)
            ))
        lat_copies.append(group)
    has_south = lat > 0
    has_north = lat < lat_n - 1
    sends = (has_south, has_north)
    gets = (has_north, has_south)

    for copy in lon_copies:
        copy.start()
    for part in (0, 1):
        @pl.when(sends[part])
        def _():
            for copy in lat_copies[part][1:]:
                copy.start()
            lat_copies[part][0].start()

        @pl.when(jnp.logical_not(gets[part]))
        def _():
            recv_lat[part] = jnp.zeros((FIELDS, rows, LANES), jnp.float32)
            recv_diag[0, part] = jnp.zeros((HALO, LANES), jnp.float32)
            recv_diag[1, part] = jnp.zeros((HALO, LANES), jnp.float32)

    for part in (0, 1):
        @pl.when(gets[part])
        def _():
            for copy in lat_copies[part]:
                copy.wait_recv()
    for copy in lon_copies:
        copy.wait_recv()

    north_side = lane_short < LANES // 2
    corners = [jnp.concatenate([recv_diag[0, part], recv_diag[1, part]], axis=0) for part in (0, 1)]

    def side(f):
        return jnp.where(north_side, recv_lat[0, f], recv_lat[1, f])

    def corner(f):
        north, south = corners
        if f > 0:
            north = pltpu.roll(north, LANES - HALO * f, 1)
            south = pltpu.roll(south, HALO * f, 1)
        return jnp.where(north_side, north, south)

    def over(k):
        return jnp.concatenate([recv_lon[0, k], recv_lon[1, k]], axis=0)

    def extended(f):
        low = [over(f * tiles + c) for c in range(tiles)] + [corner(f)]
        return jnp.concatenate(
            [jnp.concatenate([own[f], side(f)], axis=1), jnp.concatenate(low, axis=1)], axis=0
        )

    high, wide = 2 * rows, cols + LANES
    row_ext = lax.broadcasted_iota(jnp.int32, (high, wide), 0)
    col_ext = lax.broadcasted_iota(jnp.int32, (high, wide), 1)
    deep, damp, part = [extended(f) for f in range(3)]
    west_row = jnp.broadcast_to(part[high - HALO:high - HALO + 1], (rows, wide))
    sum_east = jnp.concatenate([jnp.concatenate([own[3], side(3)], axis=1), west_row], axis=0)
    strip = over(3 * tiles)
    sum_north = jnp.concatenate(
        [
            jnp.concatenate([own[4], side(4)], axis=1),
            jnp.concatenate([strip] * tiles + [corner(3)], axis=1),
        ],
        axis=0,
    )
    wet = (deep > 0.0).astype(jnp.float32)
    damp = jnp.where(damp > 0.0, damp, 1.0)
    wet_x = wet * up(wet, 0)
    wet_y = wet * up(wet, 1)
    face_x = wet_x * 0.5 * (deep + up(deep, 0))
    face_y = wet_y * 0.5 * (deep + up(deep, 1))
    at_x = jnp.logical_or(row_ext == rows - 1, row_ext == high - 1)
    at_y = jnp.logical_or(col_ext == cols - 1, col_ext == wide - 1)
    flux_x = jnp.where(at_x, wet_x * sum_east, 0.0)
    flux_y = jnp.where(at_y, wet_y * sum_north, 0.0)
    rhs = part - (flux_x - down(flux_x, 0) + flux_y - down(flux_y, 1))
    face_w, face_s = down(face_x, 0), down(face_y, 1)
    inverse = 1.0 / (damp + face_x + face_w + face_y + face_s)

    def off(p):
        return face_x * up(p, 0) + face_w * down(p, 0) + face_y * up(p, 1) + face_s * down(p, 1)

    p0 = rhs * inverse
    w1 = off(p0)
    p1 = w1 * inverse
    w2 = off(p1)
    p2 = w2 * inverse
    w3 = off(p2)
    w0, w1, w2, w3, p0, p1, p2 = [x[:rows, :cols] for x in (rhs, w1, w2, w3, p0, p1, p2)]

    lines = []
    for a, b in ((w0, p0), (w0, p1), (w1, p1), (w1, p2), (w2, p2), (w3, p2)):
        product = a * b
        folded = product[:, :LANES]
        for c in range(LANES, cols, LANES):
            folded = folded + product[:, c:c + LANES]
        lines.append(jnp.sum(folded, axis=0, keepdims=True))
    zero = jnp.zeros_like(lines[0])
    table = jnp.concatenate(lines + [zero] * (8 - len(lines)), axis=0)
    table = jnp.broadcast_to(jnp.sum(table, axis=1, keepdims=True), (8, LANES))
    pick = lax.broadcasted_iota(jnp.int32, (8, LANES), 1) == lax.broadcasted_iota(jnp.int32, (8, LANES), 0)
    row = jnp.sum(jnp.where(pick, table, 0.0), axis=0, keepdims=True)
    row_send[...] = row
    row_recv[me] = row

    def send_row(k):
        pltpu.make_async_remote_copy(
            src_ref=row_send, dst_ref=row_recv.at[me], send_sem=all_send, recv_sem=all_recv,
            device_id=peer(k), device_id_type=MESH,
        ).start()

    each_peer(send_row)

    for copy in lon_copies:
        copy.wait_send()
    for part in (0, 1):
        @pl.when(sends[part])
        def _():
            for copy in lat_copies[part]:
                copy.wait_send()

    others = row_recv.at[pl.ds(0, n - 1)]
    pltpu.make_async_copy(others, others, all_recv).wait()
    total = jnp.sum(row_recv[...], axis=0)
    nu = [jnp.broadcast_to(total[:, k:k + 1], (ROWS, LANES)) for k in range(6)]
    s, r = scalars(nu)
    for c in range(0, cols, LANES):
        part = slice(c, c + LANES)
        surface_out[:, part] = s[0] * p0[:, part] + s[1] * p1[:, part] + s[2] * p2[:, part]
        residual_out[:, part] = (r[0] * w0[:, part] + r[1] * w1[:, part]) + (r[2] * w2[:, part] + r[3] * w3[:, part])
    pltpu.make_async_copy(others, others, all_send).wait()


def solution(mesh):
    lon_n, lat_n = mesh.shape["lon"], mesh.shape["lat"]
    n = lon_n * lat_n

    def body(u_vel, v_vel, thickness, depth, sea_mask, damping, eta_prev):
        levels, rows, cols = u_vel.shape
        f32 = jnp.float32
        hbm = pl.BlockSpec(memory_space=pl.ANY)
        vmem = pl.BlockSpec(memory_space=pltpu.VMEM)
        shape = pltpu.VMEM((rows, cols), f32)
        return pl.pallas_call(
            functools.partial(kernel, lon_n, lat_n, "lon", "lat"),
            out_shape=(shape, shape),
            in_specs=[hbm] * 7,
            out_specs=(vmem, vmem),
            scratch_shapes=[
                pltpu.SMEM((levels,), f32),
                pltpu.VMEM((levels, rows, cols), f32),
                pltpu.VMEM((levels, rows, cols), f32),
                pltpu.VMEM((rows, cols), f32),
                pltpu.VMEM((rows, cols), jnp.int32),
                pltpu.VMEM((rows, cols), f32),
                pltpu.VMEM((rows, cols), f32),
                pltpu.VMEM((2, 3 * (cols // LANES) + 1, HALO, LANES), f32),
                pltpu.VMEM((2, 3 * (cols // LANES) + 1, HALO, LANES), f32),
                pltpu.VMEM((2, FIELDS, rows, LANES), f32),
                pltpu.VMEM((2, FIELDS, rows, LANES), f32),
                pltpu.VMEM((2, 2, HALO, LANES), f32),
                pltpu.VMEM((2, 2, HALO, LANES), f32),
                pltpu.VMEM((1, LANES), f32),
                pltpu.VMEM((n, 1, LANES), f32),
                pltpu.SemaphoreType.DMA((7,)),
                pltpu.SemaphoreType.DMA((8,)),
                pltpu.SemaphoreType.DMA((8,)),
                pltpu.SemaphoreType.DMA,
                pltpu.SemaphoreType.DMA,
            ],
            compiler_params=pltpu.CompilerParams(collective_id=0, has_side_effects=True),
        )(thickness, u_vel, v_vel, depth, sea_mask, damping, eta_prev)

    placed = P("lon", "lat")
    return jax.shard_map(
        body,
        mesh=mesh,
        in_specs=(P(None, "lon", "lat"), P(None, "lon", "lat"), P(), placed, placed, placed, placed),
        out_specs=(placed, placed),
        check_vma=False,
    )
```

```python
import functools
import math

import jax
import jax.numpy as jnp
from jax import lax
from jax.experimental import pallas as pl
from jax.experimental.pallas import tpu as pltpu
from jax.sharding import PartitionSpec as P

MESH = pl.DeviceIdType.MESH
HALO = 4
FIELDS = 5
LANES = 128
ROWS = 8


def scalars(nu):
    def form(c, shift):
        total = None
        for i, ci in enumerate(c):
            for j, cj in enumerate(c):
                if j < i:
                    continue
                term = ci * cj * nu[i + j + shift]
                term = term if i == j else term + term
                total = term if total is None else total + term
        return total

    def apply(c):
        out = list(c) + [None]
        for k, ck in enumerate(c):
            out[k + 1] = -ck if out[k + 1] is None else out[k + 1] - ck
        return out

    def axpy(a, x, y):
        out = []
        for k in range(max(len(x), len(y))):
            if k >= len(x):
                out.append(y[k])
            elif k >= len(y):
                out.append(a * x[k])
            else:
                out.append(y[k] + a * x[k])
        return out

    one = jnp.ones_like(nu[0])
    residual = [one]
    direction = [one]
    gamma = nu[0]
    step = gamma / (nu[0] - nu[1])
    surface = [step]
    residual = axpy(-step, apply(direction), residual)
    for _ in range(2):
        gamma_next = form(residual, 0)
        delta = gamma_next - form(residual, 1)
        ratio = gamma_next / gamma
        step = gamma_next / (delta - ratio * gamma_next / step)
        direction = axpy(ratio, direction, residual)
        surface = axpy(step, direction, surface)
        residual = axpy(-step, apply(direction), residual)
        gamma = gamma_next
    return surface, residual


def kernel(
    lon_n, lat_n, lon_axis, lat_axis,
    thick_hbm, u_hbm, v_hbm, depth_hbm, mask_hbm, damp_hbm, eta_hbm,
    surface_out, residual_out,
    thick, u_buf, v_buf, depth_v, mask_v, damp_v, eta_v,
    send_east, recv_west, send_west, recv_east, send_lat, recv_lat,
    send_diag_east, recv_diag_west, send_diag_west, recv_diag_east, row_send, row_recv,
    load_sem, halo_send, halo_recv, all_send, all_recv,
):
    levels, rows, cols = u_hbm.shape
    n = lon_n * lat_n
    lon = lax.axis_index(lon_axis)
    lat = lax.axis_index(lat_axis)
    me = lon * lat_n + lat

    def peer(k):
        flat = lax.rem(me + k, n)
        return (flat // lat_n, lax.rem(flat, lat_n))

    def each_peer(f):
        if n <= 64:
            for k in sorted(range(1, n), key=lambda k: -min(k, n - k)):
                f(k)
        else:
            lax.fori_loop(1, n, lambda k, c: (f(k), c)[1], 0)

    loads = []
    for k, (src, dst) in enumerate((
        (u_hbm, u_buf), (v_hbm, v_buf), (depth_hbm, depth_v), (mask_hbm, mask_v), (damp_hbm, damp_v), (eta_hbm, eta_v),
        (thick_hbm, thick)
    )):
        copy = pltpu.make_async_copy(src, dst, load_sem.at[k])
        copy.start()
        loads.append(copy)

    barrier = pltpu.get_barrier_semaphore()
    each_peer(lambda k: pl.semaphore_signal(barrier, inc=1, device_id=peer(k), device_id_type=MESH))

    def up(x, axis):
        return pltpu.roll(x, x.shape[axis] - 1, axis)

    def down(x, axis):
        return pltpu.roll(x, 1, axis)

    for copy in loads[2:]:
        copy.wait()
    wet_own = mask_v[...].astype(jnp.float32)
    damp_own = damp_v[...]
    deep_own = depth_v[...] * wet_own
    forced_own = wet_own * (damp_own * eta_v[...])
    row_own = lax.broadcasted_iota(jnp.int32, (rows, cols), 0)
    col_own = lax.broadcasted_iota(jnp.int32, (rows, cols), 1)
    inner_x = jnp.where(row_own < rows - 1, wet_own * up(wet_own, 0), 0.0)
    inner_y = jnp.where(col_own < cols - 1, wet_own * up(wet_own, 1), 0.0)
    scale = 1.0 / math.sqrt(levels)
    column = []
    for copy, buf in ((loads[0], u_buf), (loads[1], v_buf)):
        copy.wait()
        total = [None] * 4
        for k in range(levels):
            term = thick[k] * buf[k]
            total[k % 4] = term if total[k % 4] is None else total[k % 4] + term
        column.append(((total[0] + total[1]) + (total[2] + total[3])) * scale)
    east_own, north_own = column
    inner_x = inner_x * east_own
    inner_y = inner_y * north_own
    part_own = forced_own - (inner_x - down(inner_x, 0) + inner_y - down(inner_y, 1))
    last_east = jnp.broadcast_to(east_own[rows - 1:], (rows, cols))
    part_sent = jnp.where(row_own == 0, last_east, part_own)
    own = [deep_own, damp_own, part_own, east_own, north_own]
    tiles = cols // LANES
    lane_short = lax.broadcasted_iota(jnp.int32, (rows, LANES), 1)
    for f, (x, y) in enumerate(((deep_own, deep_own), (damp_own, damp_own), (part_own, part_sent))):
        for c in range(tiles):
            span = slice(c * LANES, (c + 1) * LANES)
            send_west[f * tiles + c] = x[:HALO, span]
            send_east[f * tiles + c] = y[:, span]
    north_last = north_own[:, cols - LANES:]
    send_west[3 * tiles] = north_last[:HALO]
    send_east[3 * tiles] = north_last

    def pack(fields, part):
        packed = None
        for f, x in enumerate(fields):
            edge = x[:, :LANES] if part == 0 else x[:, cols - LANES:]
            edge = edge if f == 0 else pltpu.roll(edge, HALO * f if part == 0 else LANES - HALO * f, 1)
            away = lane_short if part == 0 else LANES - 1 - lane_short
            packed = edge if packed is None else jnp.where(away >= HALO * f, edge, packed)
        return packed

    for part in (0, 1):
        send_diag_west[part] = pack((deep_own, damp_own, part_own, north_own), part)[:HALO]
        send_diag_east[part] = pack((deep_own, damp_own, part_sent, north_own), part)
    for f in range(FIELDS):
        send_lat[0, f] = own[f][:, :LANES]
        send_lat[1, f] = own[f][:, cols - LANES:]

    pl.semaphore_wait(barrier, n - 1)

    west = lax.rem(lon + lon_n - 1, lon_n)
    east = lax.rem(lon + 1, lon_n)

    def remote(src, dst, sem, target):
        return pltpu.make_async_remote_copy(
            src_ref=src, dst_ref=dst, send_sem=halo_send.at[sem], recv_sem=halo_recv.at[sem],
            device_id=target, device_id_type=MESH,
        )

    east_copy = remote(send_east, recv_west, 0, (east, lat))
    west_copy = remote(send_west, recv_east, 1, (west, lat))
    early, late = [], []
    for part in (0, 1):
        other = lat - 1 if part == 0 else lat + 1
        early.append([
            remote(send_diag_east.at[part], recv_diag_west.at[part], 2 + part, (east, other)),
            remote(send_lat.at[part], recv_lat.at[part], 4 + part, (lon, other)),
        ])
        late.append(remote(send_diag_west.at[part], recv_diag_east.at[part], 6 + part, (west, other)))
    has_south = lat > 0
    has_north = lat < lat_n - 1
    sends = (has_south, has_north)
    gets = (has_north, has_south)

    east_copy.start()
    for part in (0, 1):
        @pl.when(sends[part])
        def _():
            for copy in early[part]:
                copy.start()

    west_copy.start()
    for part in (0, 1):
        @pl.when(sends[part])
        def _():
            late[part].start()

        @pl.when(jnp.logical_not(gets[part]))
        def _():
            recv_lat[part] = jnp.zeros((FIELDS, rows, LANES), jnp.float32)
            recv_diag_west[part] = jnp.zeros((rows, LANES), jnp.float32)
            recv_diag_east[part] = jnp.zeros((HALO, LANES), jnp.float32)

    for part in (0, 1):
        @pl.when(gets[part])
        def _():
            for copy in early[part]:
                copy.wait_recv()
    east_copy.wait_recv()

    north_side = lane_short < LANES // 2
    high, wide = 2 * rows, cols + LANES
    row_ext = lax.broadcasted_iota(jnp.int32, (high, wide), 0)
    col_ext = lax.broadcasted_iota(jnp.int32, (high, wide), 1)

    def side(f):
        return jnp.where(north_side, recv_lat[0, f], recv_lat[1, f])

    tops = [jnp.concatenate([own[f], side(f)], axis=1) for f in range(FIELDS)]

    def krylov(over, corners, last_row, at_x):
        def corner(f):
            north, south = corners
            if f > 0:
                north = pltpu.roll(north, LANES - HALO * f, 1)
                south = pltpu.roll(south, HALO * f, 1)
            return jnp.where(north_side, north, south)

        def extended(f):
            low = [over(f * tiles + c) for c in range(tiles)] + [corner(f)]
            return jnp.concatenate([tops[f], jnp.concatenate(low, axis=1)], axis=0)

        deep, damp, known = [extended(f) for f in range(3)]
        sum_east = jnp.concatenate([tops[3], jnp.broadcast_to(last_row, (rows, wide))], axis=0)
        low_north = jnp.concatenate([over(3 * tiles)] * tiles + [corner(3)], axis=1)
        sum_north = jnp.concatenate([tops[4], low_north], axis=0)
        wet = (deep > 0.0).astype(jnp.float32)
        damp = jnp.where(damp > 0.0, damp, 1.0)
        wet_x = wet * up(wet, 0)
        wet_y = wet * up(wet, 1)
        face_x = wet_x * 0.5 * (deep + up(deep, 0))
        face_y = wet_y * 0.5 * (deep + up(deep, 1))
        at_y = jnp.logical_or(col_ext == cols - 1, col_ext == wide - 1)
        flux_x = jnp.where(at_x, wet_x * sum_east, 0.0)
        flux_y = jnp.where(at_y, wet_y * sum_north, 0.0)
        rhs = known - (flux_x - down(flux_x, 0) + flux_y - down(flux_y, 1))
        face_w, face_s = down(face_x, 0), down(face_y, 1)
        inverse = 1.0 / (damp + face_x + face_w + face_y + face_s)

        def off(p):
            return face_x * up(p, 0) + face_w * down(p, 0) + face_y * up(p, 1) + face_s * down(p, 1)

        p0 = rhs * inverse
        w1 = off(p0)
        p1 = w1 * inverse
        w2 = off(p1)
        p2 = w2 * inverse
        return rhs, w1, w2, off(p2), p0, p1, p2

    corners_west = [recv_diag_west[part] for part in (0, 1)]
    row_of_west = jnp.concatenate(
        [recv_west[2 * tiles + c][:1] for c in range(tiles)]
        + [jnp.where(
            north_side,
            pltpu.roll(corners_west[0], LANES - 2 * HALO, 1),
            pltpu.roll(corners_west[1], 2 * HALO, 1),
        )[:1]],
        axis=1,
    )
    fields = krylov(lambda k: recv_west[k], corners_west, row_of_west, row_ext == high - 1)
    upper = row_own < HALO
    w0, w1, w2, w3, p0, p1, p2 = [jnp.where(upper, x[:rows, :cols], x[rows:, :cols]) for x in fields]

    lines = []
    for a, b in ((w0, p0), (w0, p1), (w1, p1), (w1, p2), (w2, p2), (w3, p2)):
        product = a * b
        folded = product[:, :LANES]
        for c in range(LANES, cols, LANES):
            folded = folded + product[:, c:c + LANES]
        lines.append(jnp.sum(folded, axis=0, keepdims=True))
    zero = jnp.zeros_like(lines[0])
    table = jnp.concatenate(lines + [zero] * (8 - len(lines)), axis=0)
    table = jnp.broadcast_to(jnp.sum(table, axis=1, keepdims=True), (8, LANES))
    pick = lax.broadcasted_iota(jnp.int32, (8, LANES), 1) == lax.broadcasted_iota(jnp.int32, (8, LANES), 0)
    row = jnp.sum(jnp.where(pick, table, 0.0), axis=0, keepdims=True)
    row_send[...] = row
    row_recv[me] = row

    def send_row(k):
        pltpu.make_async_remote_copy(
            src_ref=row_send, dst_ref=row_recv.at[me], send_sem=all_send, recv_sem=all_recv,
            device_id=peer(k), device_id_type=MESH,
        ).start()

    each_peer(send_row)

    for part in (0, 1):
        @pl.when(gets[part])
        def _():
            late[part].wait_recv()
    west_copy.wait_recv()

    corners = [
        jnp.concatenate([recv_diag_east[part], recv_diag_west[part][rows - HALO:]], axis=0) for part in (0, 1)
    ]
    fields = krylov(
        lambda k: jnp.concatenate([recv_east[k], recv_west[k][rows - HALO:]], axis=0),
        corners, row_of_west, jnp.logical_or(row_ext == rows - 1, row_ext == high - 1),
    )
    w0, w1, w2, w3, p0, p1, p2 = [x[:rows, :cols] for x in fields]

    east_copy.wait_send()
    west_copy.wait_send()
    for part in (0, 1):
        @pl.when(sends[part])
        def _():
            for copy in early[part]:
                copy.wait_send()
            late[part].wait_send()

    others = row_recv.at[pl.ds(0, n - 1)]
    pltpu.make_async_copy(others, others, all_recv).wait()
    total = jnp.sum(row_recv[...], axis=0)
    nu = [jnp.broadcast_to(total[:, k:k + 1], (ROWS, LANES)) for k in range(6)]
    s, r = scalars(nu)
    for c in range(0, cols, LANES):
        part = slice(c, c + LANES)
        surface_out[:, part] = s[0] * p0[:, part] + s[1] * p1[:, part] + s[2] * p2[:, part]
        residual_out[:, part] = (r[0] * w0[:, part] + r[1] * w1[:, part]) + (r[2] * w2[:, part] + r[3] * w3[:, part])
    pltpu.make_async_copy(others, others, all_send).wait()


def solution(mesh):
    lon_n, lat_n = mesh.shape["lon"], mesh.shape["lat"]
    n = lon_n * lat_n

    def body(u_vel, v_vel, thickness, depth, sea_mask, damping, eta_prev):
        levels, rows, cols = u_vel.shape
        f32 = jnp.float32
        hbm = pl.BlockSpec(memory_space=pl.ANY)
        vmem = pl.BlockSpec(memory_space=pltpu.VMEM)
        shape = pltpu.VMEM((rows, cols), f32)
        return pl.pallas_call(
            functools.partial(kernel, lon_n, lat_n, "lon", "lat"),
            out_shape=(shape, shape),
            in_specs=[hbm] * 7,
            out_specs=(vmem, vmem),
            scratch_shapes=[
                pltpu.SMEM((levels,), f32),
                pltpu.VMEM((levels, rows, cols), f32),
                pltpu.VMEM((levels, rows, cols), f32),
                pltpu.VMEM((rows, cols), f32),
                pltpu.VMEM((rows, cols), jnp.int32),
                pltpu.VMEM((rows, cols), f32),
                pltpu.VMEM((rows, cols), f32),
                pltpu.VMEM((3 * (cols // LANES) + 1, rows, LANES), f32),
                pltpu.VMEM((3 * (cols // LANES) + 1, rows, LANES), f32),
                pltpu.VMEM((3 * (cols // LANES) + 1, HALO, LANES), f32),
                pltpu.VMEM((3 * (cols // LANES) + 1, HALO, LANES), f32),
                pltpu.VMEM((2, FIELDS, rows, LANES), f32),
                pltpu.VMEM((2, FIELDS, rows, LANES), f32),
                pltpu.VMEM((2, rows, LANES), f32),
                pltpu.VMEM((2, rows, LANES), f32),
                pltpu.VMEM((2, HALO, LANES), f32),
                pltpu.VMEM((2, HALO, LANES), f32),
                pltpu.VMEM((1, LANES), f32),
                pltpu.VMEM((n, 1, LANES), f32),
                pltpu.SemaphoreType.DMA((7,)),
                pltpu.SemaphoreType.DMA((8,)),
                pltpu.SemaphoreType.DMA((8,)),
                pltpu.SemaphoreType.DMA,
                pltpu.SemaphoreType.DMA,
            ],
            compiler_params=pltpu.CompilerParams(collective_id=0, has_side_effects=True),
        )(thickness, u_vel, v_vel, depth, sea_mask, damping, eta_prev)

    placed = P("lon", "lat")
    return jax.shard_map(
        body,
        mesh=mesh,
        in_specs=(P(None, "lon", "lat"), P(None, "lon", "lat"), P(), placed, placed, placed, placed),
        out_specs=(placed, placed),
        check_vma=False,
    )
```

```python
import functools
import math

import jax
import jax.numpy as jnp
from jax import lax
from jax.experimental import pallas as pl
from jax.experimental.pallas import tpu as pltpu
from jax.sharding import PartitionSpec as P

MESH = pl.DeviceIdType.MESH
HALO = 4
FIELDS = 5
LANES = 128
ROWS = 8


def scalars(nu):
    def form(c, shift):
        total = None
        for i, ci in enumerate(c):
            for j, cj in enumerate(c):
                if j < i:
                    continue
                term = ci * cj * nu[i + j + shift]
                term = term if i == j else term + term
                total = term if total is None else total + term
        return total

    def apply(c):
        out = list(c) + [None]
        for k, ck in enumerate(c):
            out[k + 1] = -ck if out[k + 1] is None else out[k + 1] - ck
        return out

    def axpy(a, x, y):
        out = []
        for k in range(max(len(x), len(y))):
            if k >= len(x):
                out.append(y[k])
            elif k >= len(y):
                out.append(a * x[k])
            else:
                out.append(y[k] + a * x[k])
        return out

    one = jnp.ones_like(nu[0])
    residual = [one]
    direction = [one]
    gamma = nu[0]
    step = gamma / (nu[0] - nu[1])
    surface = [step]
    residual = axpy(-step, apply(direction), residual)
    for _ in range(2):
        gamma_next = form(residual, 0)
        delta = gamma_next - form(residual, 1)
        ratio = gamma_next / gamma
        step = gamma_next / (delta - ratio * gamma_next / step)
        direction = axpy(ratio, direction, residual)
        surface = axpy(step, direction, surface)
        residual = axpy(-step, apply(direction), residual)
        gamma = gamma_next
    return surface, residual


def kernel(
    lon_n, lat_n, lon_axis, lat_axis,
    thick_hbm, u_hbm, v_hbm, depth_hbm, mask_hbm, damp_hbm, eta_hbm,
    both_out,
    thick, u_buf, v_buf, depth_v, mask_v, damp_v, eta_v,
    send_east, recv_west, send_west, recv_east, send_lat, recv_lat,
    send_diag_east, recv_diag_west, send_diag_west, recv_diag_east, row_send, row_recv,
    load_sem, halo_send, halo_recv, all_send, all_recv,
):
    levels, rows, cols = u_hbm.shape
    n = lon_n * lat_n
    lon = lax.axis_index(lon_axis)
    lat = lax.axis_index(lat_axis)
    me = lon * lat_n + lat

    def peer(k):
        flat = lax.rem(me + k, n)
        return (flat // lat_n, lax.rem(flat, lat_n))

    def each_peer(f):
        if n <= 64:
            for k in sorted(range(1, n), key=lambda k: min(k, n - k)):
                f(k)
        else:
            lax.fori_loop(1, n, lambda k, c: (f(k), c)[1], 0)

    loads = []
    for k, (src, dst) in enumerate((
        (u_hbm, u_buf), (v_hbm, v_buf), (depth_hbm, depth_v), (mask_hbm, mask_v), (damp_hbm, damp_v), (eta_hbm, eta_v),
        (thick_hbm, thick)
    )):
        copy = pltpu.make_async_copy(src, dst, load_sem.at[k])
        copy.start()
        loads.append(copy)

    barrier = pltpu.get_barrier_semaphore()
    each_peer(lambda k: pl.semaphore_signal(barrier, inc=1, device_id=peer(k), device_id_type=MESH))

    def up(x, axis):
        return pltpu.roll(x, x.shape[axis] - 1, axis)

    def down(x, axis):
        return pltpu.roll(x, 1, axis)

    for copy in loads[2:]:
        copy.wait()
    wet_own = mask_v[...].astype(jnp.float32)
    damp_own = damp_v[...]
    deep_own = depth_v[...] * wet_own
    forced_own = wet_own * (damp_own * eta_v[...])
    row_own = lax.broadcasted_iota(jnp.int32, (rows, cols), 0)
    col_own = lax.broadcasted_iota(jnp.int32, (rows, cols), 1)
    inner_x = jnp.where(row_own < rows - 1, wet_own * up(wet_own, 0), 0.0)
    inner_y = jnp.where(col_own < cols - 1, wet_own * up(wet_own, 1), 0.0)
    scale = 1.0 / math.sqrt(levels)
    column = []
    for copy, buf in ((loads[0], u_buf), (loads[1], v_buf)):
        copy.wait()
        total = [None] * 4
        for k in range(levels):
            term = thick[k] * buf[k]
            total[k % 4] = term if total[k % 4] is None else total[k % 4] + term
        column.append(((total[0] + total[1]) + (total[2] + total[3])) * scale)
    east_own, north_own = column
    inner_x = inner_x * east_own
    inner_y = inner_y * north_own
    part_own = forced_own - (inner_x - down(inner_x, 0) + inner_y - down(inner_y, 1))
    last_east = jnp.broadcast_to(east_own[rows - 1:], (rows, cols))
    part_sent = jnp.where(row_own == 0, last_east, part_own)
    own = [deep_own, damp_own, part_own, east_own, north_own]
    tiles = cols // LANES
    lane_short = lax.broadcasted_iota(jnp.int32, (rows, LANES), 1)
    for f, (x, y) in enumerate(((deep_own, deep_own), (damp_own, damp_own), (part_own, part_sent))):
        for c in range(tiles):
            span = slice(c * LANES, (c + 1) * LANES)
            send_west[f * tiles + c] = x[:HALO, span]
            send_east[f * tiles + c] = y[:, span]
    north_last = north_own[:, cols - LANES:]
    send_west[3 * tiles] = north_last[:HALO]
    send_east[3 * tiles] = north_last

    def pack(fields, part):
        packed = None
        for f, x in enumerate(fields):
            edge = x[:, :LANES] if part == 0 else x[:, cols - LANES:]
            edge = edge if f == 0 else pltpu.roll(edge, HALO * f if part == 0 else LANES - HALO * f, 1)
            away = lane_short if part == 0 else LANES - 1 - lane_short
            packed = edge if packed is None else jnp.where(away >= HALO * f, edge, packed)
        return packed

    for part in (0, 1):
        send_diag_west[part] = pack((deep_own, damp_own, part_own, north_own), part)[:HALO]
        send_diag_east[part] = pack((deep_own, damp_own, part_sent, north_own), part)
    for f in range(FIELDS):
        send_lat[0, f] = own[f][:, :LANES]
        send_lat[1, f] = own[f][:, cols - LANES:]

    pl.semaphore_wait(barrier, n - 1)

    west = lax.rem(lon + lon_n - 1, lon_n)
    east = lax.rem(lon + 1, lon_n)

    def remote(src, dst, sem, target):
        return pltpu.make_async_remote_copy(
            src_ref=src, dst_ref=dst, send_sem=halo_send.at[sem], recv_sem=halo_recv.at[sem],
            device_id=target, device_id_type=MESH,
        )

    east_copy = remote(send_east, recv_west, 0, (east, lat))
    west_copy = remote(send_west, recv_east, 1, (west, lat))
    early, late = [], []
    for part in (0, 1):
        other = lat - 1 if part == 0 else lat + 1
        early.append([
            remote(send_diag_east.at[part], recv_diag_west.at[part], 2 + part, (east, other)),
            remote(send_lat.at[part], recv_lat.at[part], 4 + part, (lon, other)),
        ])
        late.append(remote(send_diag_west.at[part], recv_diag_east.at[part], 6 + part, (west, other)))
    has_south = lat > 0
    has_north = lat < lat_n - 1
    sends = (has_south, has_north)
    gets = (has_north, has_south)

    east_copy.start()
    for part in (0, 1):
        @pl.when(sends[part])
        def _():
            for copy in early[part]:
                copy.start()

    for part in (0, 1):
        @pl.when(jnp.logical_not(gets[part]))
        def _():
            recv_lat[part] = jnp.zeros((FIELDS, rows, LANES), jnp.float32)
            recv_diag_west[part] = jnp.zeros((rows, LANES), jnp.float32)
            recv_diag_east[part] = jnp.zeros((HALO, LANES), jnp.float32)

    for part in (0, 1):
        @pl.when(gets[part])
        def _():
            for copy in early[part]:
                copy.wait_recv()
    east_copy.wait_recv()

    north_side = lane_short < LANES // 2
    high, wide = 2 * rows, cols + LANES
    row_ext = lax.broadcasted_iota(jnp.int32, (high, wide), 0)
    col_ext = lax.broadcasted_iota(jnp.int32, (high, wide), 1)

    def side(f):
        return jnp.where(north_side, recv_lat[0, f], recv_lat[1, f])

    tops = [jnp.concatenate([own[f], side(f)], axis=1) for f in range(FIELDS)]

    west_copy.start()
    for part in (0, 1):
        @pl.when(sends[part])
        def _():
            late[part].start()

    def krylov(over, corners, last_row, at_x):
        def corner(f):
            north, south = corners
            if f > 0:
                north = pltpu.roll(north, LANES - HALO * f, 1)
                south = pltpu.roll(south, HALO * f, 1)
            return jnp.where(north_side, north, south)

        def extended(f):
            low = [over(f * tiles + c) for c in range(tiles)] + [corner(f)]
            return jnp.concatenate([tops[f], jnp.concatenate(low, axis=1)], axis=0)

        deep, damp, known = [extended(f) for f in range(3)]
        sum_east = jnp.concatenate([tops[3], jnp.broadcast_to(last_row, (rows, wide))], axis=0)
        low_north = jnp.concatenate([over(3 * tiles)] * tiles + [corner(3)], axis=1)
        sum_north = jnp.concatenate([tops[4], low_north], axis=0)
        wet = (deep > 0.0).astype(jnp.float32)
        damp = jnp.where(damp > 0.0, damp, 1.0)
        wet_x = wet * up(wet, 0)
        wet_y = wet * up(wet, 1)
        face_x = wet_x * 0.5 * (deep + up(deep, 0))
        face_y = wet_y * 0.5 * (deep + up(deep, 1))
        at_y = jnp.logical_or(col_ext == cols - 1, col_ext == wide - 1)
        flux_x = jnp.where(at_x, wet_x * sum_east, 0.0)
        flux_y = jnp.where(at_y, wet_y * sum_north, 0.0)
        rhs = known - (flux_x - down(flux_x, 0) + flux_y - down(flux_y, 1))
        face_w, face_s = down(face_x, 0), down(face_y, 1)
        inverse = 1.0 / (damp + face_x + face_w + face_y + face_s)

        def off(p):
            return face_x * up(p, 0) + face_w * down(p, 0) + face_y * up(p, 1) + face_s * down(p, 1)

        p0 = rhs * inverse
        w1 = off(p0)
        p1 = w1 * inverse
        w2 = off(p1)
        p2 = w2 * inverse
        return rhs, w1, w2, off(p2), p0, p1, p2

    corners_west = [recv_diag_west[part] for part in (0, 1)]
    row_of_west = jnp.concatenate(
        [recv_west[2 * tiles + c][:1] for c in range(tiles)]
        + [jnp.where(
            north_side,
            pltpu.roll(corners_west[0], LANES - 2 * HALO, 1),
            pltpu.roll(corners_west[1], 2 * HALO, 1),
        )[:1]],
        axis=1,
    )
    fields = krylov(lambda k: recv_west[k], corners_west, row_of_west, row_ext == high - 1)
    upper = row_own < HALO
    w0, w1, w2, w3, p0, p1, p2 = [jnp.where(upper, x[:rows, :cols], x[rows:, :cols]) for x in fields]

    lines = []
    for a, b in ((w0, p0), (w0, p1), (w1, p1), (w1, p2), (w2, p2), (w3, p2)):
        product = a * b
        folded = product[:, :LANES]
        for c in range(LANES, cols, LANES):
            folded = folded + product[:, c:c + LANES]
        lines.append(jnp.sum(folded, axis=0, keepdims=True))
    zero = jnp.zeros_like(lines[0])
    table = jnp.concatenate(lines + [zero] * (8 - len(lines)), axis=0)
    table = jnp.broadcast_to(jnp.sum(table, axis=1, keepdims=True), (8, LANES))
    pick = lax.broadcasted_iota(jnp.int32, (8, LANES), 1) == lax.broadcasted_iota(jnp.int32, (8, LANES), 0)
    row = jnp.sum(jnp.where(pick, table, 0.0), axis=0, keepdims=True)
    row_send[...] = row
    row_recv[me] = row

    def send_row(k):
        pltpu.make_async_remote_copy(
            src_ref=row_send, dst_ref=row_recv.at[me], send_sem=all_send, recv_sem=all_recv,
            device_id=peer(k), device_id_type=MESH,
        ).start()

    each_peer(send_row)

    for part in (0, 1):
        @pl.when(gets[part])
        def _():
            late[part].wait_recv()
    west_copy.wait_recv()

    corners = [
        jnp.concatenate([recv_diag_east[part], recv_diag_west[part][rows - HALO:]], axis=0) for part in (0, 1)
    ]
    fields = krylov(
        lambda k: jnp.concatenate([recv_east[k], recv_west[k][rows - HALO:]], axis=0),
        corners, row_of_west, jnp.logical_or(row_ext == rows - 1, row_ext == high - 1),
    )
    w0, w1, w2, w3, p0, p1, p2 = [x[:rows, :cols] for x in fields]

    east_copy.wait_send()
    west_copy.wait_send()
    for part in (0, 1):
        @pl.when(sends[part])
        def _():
            for copy in early[part]:
                copy.wait_send()
            late[part].wait_send()

    others = row_recv.at[pl.ds(0, n - 1)]
    pltpu.make_async_copy(others, others, all_recv).wait()
    total = jnp.sum(row_recv[...], axis=0)
    nu = [jnp.broadcast_to(total[:, k:k + 1], (ROWS, LANES)) for k in range(6)]
    s, r = scalars(nu)
    for c in range(0, cols, LANES):
        part = slice(c, c + LANES)
        both_out[0, :, part] = s[0] * p0[:, part] + s[1] * p1[:, part] + s[2] * p2[:, part]
        both_out[1, :, part] = (r[0] * w0[:, part] + r[1] * w1[:, part]) + (r[2] * w2[:, part] + r[3] * w3[:, part])
    pltpu.make_async_copy(others, others, all_send).wait()


def solution(mesh):
    lon_n, lat_n = mesh.shape["lon"], mesh.shape["lat"]
    n = lon_n * lat_n

    def body(u_vel, v_vel, thickness, depth, sea_mask, damping, eta_prev):
        levels, rows, cols = u_vel.shape
        f32 = jnp.float32
        hbm = pl.BlockSpec(memory_space=pl.ANY)
        vmem = pl.BlockSpec(memory_space=pltpu.VMEM)
        shape = pltpu.VMEM((2, rows, cols), f32)
        both = pl.pallas_call(
            functools.partial(kernel, lon_n, lat_n, "lon", "lat"),
            out_shape=shape,
            in_specs=[hbm] * 7,
            out_specs=vmem,
            scratch_shapes=[
                pltpu.SMEM((levels,), f32),
                pltpu.VMEM((levels, rows, cols), f32),
                pltpu.VMEM((levels, rows, cols), f32),
                pltpu.VMEM((rows, cols), f32),
                pltpu.VMEM((rows, cols), jnp.int32),
                pltpu.VMEM((rows, cols), f32),
                pltpu.VMEM((rows, cols), f32),
                pltpu.VMEM((3 * (cols // LANES) + 1, rows, LANES), f32),
                pltpu.VMEM((3 * (cols // LANES) + 1, rows, LANES), f32),
                pltpu.VMEM((3 * (cols // LANES) + 1, HALO, LANES), f32),
                pltpu.VMEM((3 * (cols // LANES) + 1, HALO, LANES), f32),
                pltpu.VMEM((2, FIELDS, rows, LANES), f32),
                pltpu.VMEM((2, FIELDS, rows, LANES), f32),
                pltpu.VMEM((2, rows, LANES), f32),
                pltpu.VMEM((2, rows, LANES), f32),
                pltpu.VMEM((2, HALO, LANES), f32),
                pltpu.VMEM((2, HALO, LANES), f32),
                pltpu.VMEM((1, LANES), f32),
                pltpu.VMEM((n, 1, LANES), f32),
                pltpu.SemaphoreType.DMA((7,)),
                pltpu.SemaphoreType.DMA((8,)),
                pltpu.SemaphoreType.DMA((8,)),
                pltpu.SemaphoreType.DMA,
                pltpu.SemaphoreType.DMA,
            ],
            compiler_params=pltpu.CompilerParams(collective_id=0, has_side_effects=True),
        )(thickness, u_vel, v_vel, depth, sea_mask, damping, eta_prev)
        return both[0], both[1]


    placed = P("lon", "lat")
    return jax.shard_map(
        body,
        mesh=mesh,
        in_specs=(P(None, "lon", "lat"), P(None, "lon", "lat"), P(), placed, placed, placed, placed),
        out_specs=(placed, placed),
        check_vma=False,
    )
```

```python
import functools
import math

import jax
import jax.numpy as jnp
from jax import lax
from jax.experimental import pallas as pl
from jax.experimental.pallas import tpu as pltpu
from jax.sharding import PartitionSpec as P

MESH = pl.DeviceIdType.MESH
HALO = 4
FIELDS = 5
LANES = 128
ROWS = 8


def scalars(nu):
    def form(c, shift):
        total = None
        for i, ci in enumerate(c):
            for j, cj in enumerate(c):
                if j < i:
                    continue
                term = ci * cj * nu[i + j + shift]
                term = term if i == j else term + term
                total = term if total is None else total + term
        return total

    def apply(c):
        out = list(c) + [None]
        for k, ck in enumerate(c):
            out[k + 1] = -ck if out[k + 1] is None else out[k + 1] - ck
        return out

    def axpy(a, x, y):
        out = []
        for k in range(max(len(x), len(y))):
            if k >= len(x):
                out.append(y[k])
            elif k >= len(y):
                out.append(a * x[k])
            else:
                out.append(y[k] + a * x[k])
        return out

    one = jnp.ones_like(nu[0])
    residual = [one]
    direction = [one]
    under = nu[0] - nu[1]
    step = nu[0] / under
    inverse = 1.0 / nu[0]
    step_inverse = under * inverse
    surface = [step]
    residual = axpy(-step, apply(direction), residual)
    for _ in range(2):
        gamma_next = form(residual, 0)
        delta = gamma_next - form(residual, 1)
        ratio = gamma_next * inverse
        under = delta - ratio * gamma_next * step_inverse
        step = gamma_next / under
        inverse = 1.0 / gamma_next
        step_inverse = under * inverse
        direction = axpy(ratio, direction, residual)
        surface = axpy(step, direction, surface)
        residual = axpy(-step, apply(direction), residual)
    return surface, residual


def kernel(
    lon_n, lat_n, lon_axis, lat_axis,
    thick_hbm, u_hbm, v_hbm, depth_hbm, mask_hbm, damp_hbm, eta_hbm,
    both_out,
    thick, u_buf, v_buf, depth_v, mask_v, damp_v, eta_v,
    send_east, recv_west, send_west, recv_east, send_lat, recv_lat,
    send_diag_east, recv_diag_west, send_diag_west, recv_diag_east, row_send, row_recv,
    load_sem, halo_send, halo_recv, all_send, all_recv,
):
    levels, rows, cols = u_hbm.shape
    n = lon_n * lat_n
    lon = lax.axis_index(lon_axis)
    lat = lax.axis_index(lat_axis)
    me = lon * lat_n + lat

    def peer(k):
        flat = lax.rem(me + k, n)
        return (flat // lat_n, lax.rem(flat, lat_n))

    def each_peer(f):
        if n <= 64:
            for k in sorted(range(1, n), key=lambda k: min(k, n - k)):
                f(k)
        else:
            lax.fori_loop(1, n, lambda k, c: (f(k), c)[1], 0)

    loads = []
    for k, (src, dst) in enumerate((
        (u_hbm, u_buf), (v_hbm, v_buf), (depth_hbm, depth_v), (mask_hbm, mask_v), (damp_hbm, damp_v), (eta_hbm, eta_v),
        (thick_hbm, thick)
    )):
        copy = pltpu.make_async_copy(src, dst, load_sem.at[k])
        copy.start()
        loads.append(copy)

    barrier = pltpu.get_barrier_semaphore()
    each_peer(lambda k: pl.semaphore_signal(barrier, inc=1, device_id=peer(k), device_id_type=MESH))

    def up(x, axis):
        return pltpu.roll(x, x.shape[axis] - 1, axis)

    def down(x, axis):
        return pltpu.roll(x, 1, axis)

    for copy in loads[2:]:
        copy.wait()
    wet_own = mask_v[...].astype(jnp.float32)
    damp_own = damp_v[...]
    deep_own = depth_v[...] * wet_own
    forced_own = wet_own * (damp_own * eta_v[...])
    row_own = lax.broadcasted_iota(jnp.int32, (rows, cols), 0)
    col_own = lax.broadcasted_iota(jnp.int32, (rows, cols), 1)
    inner_x = jnp.where(row_own < rows - 1, wet_own * up(wet_own, 0), 0.0)
    inner_y = jnp.where(col_own < cols - 1, wet_own * up(wet_own, 1), 0.0)
    scale = 1.0 / math.sqrt(levels)
    column = []
    for copy, buf in ((loads[0], u_buf), (loads[1], v_buf)):
        copy.wait()
        total = [None] * 4
        for k in range(levels):
            term = thick[k] * buf[k]
            total[k % 4] = term if total[k % 4] is None else total[k % 4] + term
        column.append(((total[0] + total[1]) + (total[2] + total[3])) * scale)
    east_own, north_own = column
    inner_x = inner_x * east_own
    inner_y = inner_y * north_own
    part_own = forced_own - (inner_x - down(inner_x, 0) + inner_y - down(inner_y, 1))
    last_east = jnp.broadcast_to(east_own[rows - 1:], (rows, cols))
    part_sent = jnp.where(row_own == 0, last_east, part_own)
    own = [deep_own, damp_own, part_own, east_own, north_own]
    tiles = cols // LANES
    lane_short = lax.broadcasted_iota(jnp.int32, (rows, LANES), 1)
    for f, (x, y) in enumerate(((deep_own, deep_own), (damp_own, damp_own), (part_own, part_sent))):
        for c in range(tiles):
            span = slice(c * LANES, (c + 1) * LANES)
            send_west[f * tiles + c] = x[:HALO, span]
            send_east[f * tiles + c] = y[:, span]
    north_last = north_own[:, cols - LANES:]
    send_west[3 * tiles] = north_last[:HALO]
    send_east[3 * tiles] = north_last

    def pack(fields, part):
        packed = None
        for f, x in enumerate(fields):
            edge = x[:, :LANES] if part == 0 else x[:, cols - LANES:]
            edge = edge if f == 0 else pltpu.roll(edge, HALO * f if part == 0 else LANES - HALO * f, 1)
            away = lane_short if part == 0 else LANES - 1 - lane_short
            packed = edge if packed is None else jnp.where(away >= HALO * f, edge, packed)
        return packed

    for part in (0, 1):
        send_diag_west[part] = pack((deep_own, damp_own, part_own, north_own), part)[:HALO]
        send_diag_east[part] = pack((deep_own, damp_own, part_sent, north_own), part)
    for f in range(FIELDS):
        send_lat[0, f] = own[f][:, :LANES]
        send_lat[1, f] = own[f][:, cols - LANES:]

    pl.semaphore_wait(barrier, n - 1)

    west = lax.rem(lon + lon_n - 1, lon_n)
    east = lax.rem(lon + 1, lon_n)

    def remote(src, dst, sem, target):
        return pltpu.make_async_remote_copy(
            src_ref=src, dst_ref=dst, send_sem=halo_send.at[sem], recv_sem=halo_recv.at[sem],
            device_id=target, device_id_type=MESH,
        )

    east_copy = remote(send_east, recv_west, 0, (east, lat))
    west_copy = remote(send_west, recv_east, 1, (west, lat))
    early, late = [], []
    for part in (0, 1):
        other = lat - 1 if part == 0 else lat + 1
        early.append([
            remote(send_diag_east.at[part], recv_diag_west.at[part], 2 + part, (east, other)),
            remote(send_lat.at[part], recv_lat.at[part], 4 + part, (lon, other)),
        ])
        late.append(remote(send_diag_west.at[part], recv_diag_east.at[part], 6 + part, (west, other)))
    has_south = lat > 0
    has_north = lat < lat_n - 1
    sends = (has_south, has_north)
    gets = (has_north, has_south)

    east_copy.start()
    for part in (0, 1):
        @pl.when(sends[part])
        def _():
            for copy in early[part]:
                copy.start()

    for part in (0, 1):
        @pl.when(jnp.logical_not(gets[part]))
        def _():
            recv_lat[part] = jnp.zeros((FIELDS, rows, LANES), jnp.float32)
            recv_diag_west[part] = jnp.zeros((rows, LANES), jnp.float32)
            recv_diag_east[part] = jnp.zeros((HALO, LANES), jnp.float32)

    for part in (0, 1):
        @pl.when(gets[part])
        def _():
            for copy in early[part]:
                copy.wait_recv()
    east_copy.wait_recv()

    north_side = lane_short < LANES // 2
    high, wide = 2 * rows, cols + LANES
    row_ext = lax.broadcasted_iota(jnp.int32, (high, wide), 0)
    col_ext = lax.broadcasted_iota(jnp.int32, (high, wide), 1)

    def side(f):
        return jnp.where(north_side, recv_lat[0, f], recv_lat[1, f])

    tops = [jnp.concatenate([own[f], side(f)], axis=1) for f in range(FIELDS)]

    west_copy.start()
    for part in (0, 1):
        @pl.when(sends[part])
        def _():
            late[part].start()

    def krylov(over, corners, last_row, at_x):
        def corner(f):
            north, south = corners
            if f > 0:
                north = pltpu.roll(north, LANES - HALO * f, 1)
                south = pltpu.roll(south, HALO * f, 1)
            return jnp.where(north_side, north, south)

        def extended(f):
            low = [over(f * tiles + c) for c in range(tiles)] + [corner(f)]
            return jnp.concatenate([tops[f], jnp.concatenate(low, axis=1)], axis=0)

        deep, damp, known = [extended(f) for f in range(3)]
        sum_east = jnp.concatenate([tops[3], jnp.broadcast_to(last_row, (rows, wide))], axis=0)
        low_north = jnp.concatenate([over(3 * tiles)] * tiles + [corner(3)], axis=1)
        sum_north = jnp.concatenate([tops[4], low_north], axis=0)
        wet = (deep > 0.0).astype(jnp.float32)
        damp = jnp.where(damp > 0.0, damp, 1.0)
        wet_x = wet * up(wet, 0)
        wet_y = wet * up(wet, 1)
        face_x = wet_x * 0.5 * (deep + up(deep, 0))
        face_y = wet_y * 0.5 * (deep + up(deep, 1))
        at_y = jnp.logical_or(col_ext == cols - 1, col_ext == wide - 1)
        flux_x = jnp.where(at_x, wet_x * sum_east, 0.0)
        flux_y = jnp.where(at_y, wet_y * sum_north, 0.0)
        rhs = known - (flux_x - down(flux_x, 0) + flux_y - down(flux_y, 1))
        face_w, face_s = down(face_x, 0), down(face_y, 1)
        inverse = 1.0 / (damp + face_x + face_w + face_y + face_s)

        def off(p):
            return face_x * up(p, 0) + face_w * down(p, 0) + face_y * up(p, 1) + face_s * down(p, 1)

        p0 = rhs * inverse
        w1 = off(p0)
        p1 = w1 * inverse
        w2 = off(p1)
        p2 = w2 * inverse
        return rhs, w1, w2, off(p2), p0, p1, p2

    corners_west = [recv_diag_west[part] for part in (0, 1)]
    row_of_west = jnp.concatenate(
        [recv_west[2 * tiles + c][:1] for c in range(tiles)]
        + [jnp.where(
            north_side,
            pltpu.roll(corners_west[0], LANES - 2 * HALO, 1),
            pltpu.roll(corners_west[1], 2 * HALO, 1),
        )[:1]],
        axis=1,
    )
    fields = krylov(lambda k: recv_west[k], corners_west, row_of_west, row_ext == high - 1)
    upper = row_own < HALO
    w0, w1, w2, w3, p0, p1, p2 = [jnp.where(upper, x[:rows, :cols], x[rows:, :cols]) for x in fields]

    lines = []
    for a, b in ((w0, p0), (w0, p1), (w1, p1), (w1, p2), (w2, p2), (w3, p2)):
        product = a * b
        folded = product[:, :LANES]
        for c in range(LANES, cols, LANES):
            folded = folded + product[:, c:c + LANES]
        lines.append(jnp.sum(folded, axis=0, keepdims=True))
    zero = jnp.zeros_like(lines[0])
    table = jnp.concatenate(lines + [zero] * (8 - len(lines)), axis=0)
    table = jnp.broadcast_to(jnp.sum(table, axis=1, keepdims=True), (8, LANES))
    pick = lax.broadcasted_iota(jnp.int32, (8, LANES), 1) == lax.broadcasted_iota(jnp.int32, (8, LANES), 0)
    row = jnp.sum(jnp.where(pick, table, 0.0), axis=0, keepdims=True)
    row_send[...] = row
    row_recv[me] = row

    def send_row(k):
        pltpu.make_async_remote_copy(
            src_ref=row_send, dst_ref=row_recv.at[me], send_sem=all_send, recv_sem=all_recv,
            device_id=peer(k), device_id_type=MESH,
        ).start()

    each_peer(send_row)

    for part in (0, 1):
        @pl.when(gets[part])
        def _():
            late[part].wait_recv()
    west_copy.wait_recv()

    corners = [
        jnp.concatenate([recv_diag_east[part], recv_diag_west[part][rows - HALO:]], axis=0) for part in (0, 1)
    ]
    fields = krylov(
        lambda k: jnp.concatenate([recv_east[k], recv_west[k][rows - HALO:]], axis=0),
        corners, row_of_west, jnp.logical_or(row_ext == rows - 1, row_ext == high - 1),
    )
    w0, w1, w2, w3, p0, p1, p2 = [x[:rows, :cols] for x in fields]

    east_copy.wait_send()
    west_copy.wait_send()
    for part in (0, 1):
        @pl.when(sends[part])
        def _():
            for copy in early[part]:
                copy.wait_send()
            late[part].wait_send()

    others = row_recv.at[pl.ds(0, n - 1)]
    pltpu.make_async_copy(others, others, all_recv).wait()
    if n <= 64:
        heap = [row_recv[k] for k in range(n)]
        while len(heap) > 1:
            heap = [a + b for a, b in zip(heap[::2], heap[1::2])] + heap[len(heap) - len(heap) % 2:]
        total = heap[0]
    else:
        total = jnp.sum(row_recv[...], axis=0)
    nu = [jnp.broadcast_to(total[:, k:k + 1], (ROWS, LANES)) for k in range(6)]
    s, r = scalars(nu)
    for c in range(0, cols, LANES):
        part = slice(c, c + LANES)
        both_out[0, :, part] = s[0] * p0[:, part] + s[1] * p1[:, part] + s[2] * p2[:, part]
        both_out[1, :, part] = (r[0] * w0[:, part] + r[1] * w1[:, part]) + (r[2] * w2[:, part] + r[3] * w3[:, part])
    pltpu.make_async_copy(others, others, all_send).wait()


def solution(mesh):
    lon_n, lat_n = mesh.shape["lon"], mesh.shape["lat"]
    n = lon_n * lat_n

    def body(u_vel, v_vel, thickness, depth, sea_mask, damping, eta_prev):
        levels, rows, cols = u_vel.shape
        f32 = jnp.float32
        hbm = pl.BlockSpec(memory_space=pl.ANY)
        vmem = pl.BlockSpec(memory_space=pltpu.VMEM)
        shape = pltpu.VMEM((2, rows, cols), f32)
        both = pl.pallas_call(
            functools.partial(kernel, lon_n, lat_n, "lon", "lat"),
            out_shape=shape,
            in_specs=[hbm] * 7,
            out_specs=vmem,
            scratch_shapes=[
                pltpu.SMEM((levels,), f32),
                pltpu.VMEM((levels, rows, cols), f32),
                pltpu.VMEM((levels, rows, cols), f32),
                pltpu.VMEM((rows, cols), f32),
                pltpu.VMEM((rows, cols), jnp.int32),
                pltpu.VMEM((rows, cols), f32),
                pltpu.VMEM((rows, cols), f32),
                pltpu.VMEM((3 * (cols // LANES) + 1, rows, LANES), f32),
                pltpu.VMEM((3 * (cols // LANES) + 1, rows, LANES), f32),
                pltpu.VMEM((3 * (cols // LANES) + 1, HALO, LANES), f32),
                pltpu.VMEM((3 * (cols // LANES) + 1, HALO, LANES), f32),
                pltpu.VMEM((2, FIELDS, rows, LANES), f32),
                pltpu.VMEM((2, FIELDS, rows, LANES), f32),
                pltpu.VMEM((2, rows, LANES), f32),
                pltpu.VMEM((2, rows, LANES), f32),
                pltpu.VMEM((2, HALO, LANES), f32),
                pltpu.VMEM((2, HALO, LANES), f32),
                pltpu.VMEM((1, LANES), f32),
                pltpu.VMEM((n, 1, LANES), f32),
                pltpu.SemaphoreType.DMA((7,)),
                pltpu.SemaphoreType.DMA((8,)),
                pltpu.SemaphoreType.DMA((8,)),
                pltpu.SemaphoreType.DMA,
                pltpu.SemaphoreType.DMA,
            ],
            compiler_params=pltpu.CompilerParams(collective_id=0, has_side_effects=True),
        )(thickness, u_vel, v_vel, depth, sea_mask, damping, eta_prev)
        return both[0], both[1]


    placed = P("lon", "lat")
    return jax.shard_map(
        body,
        mesh=mesh,
        in_specs=(P(None, "lon", "lat"), P(None, "lon", "lat"), P(), placed, placed, placed, placed),
        out_specs=(placed, placed),
        check_vma=False,
    )
```

```python
import functools
import math

import jax
import jax.numpy as jnp
from jax import lax
from jax.experimental import pallas as pl
from jax.experimental.pallas import tpu as pltpu
from jax.sharding import PartitionSpec as P

MESH = pl.DeviceIdType.MESH
HALO = 4
FIELDS = 5
LANES = 128
ROWS = 8


def scalars(nu):
    def form(c, shift):
        total = None
        for i, ci in enumerate(c):
            for j, cj in enumerate(c):
                if j < i:
                    continue
                term = ci * cj * nu[i + j + shift]
                term = term if i == j else term + term
                total = term if total is None else total + term
        return total

    def apply(c):
        out = list(c) + [None]
        for k, ck in enumerate(c):
            out[k + 1] = -ck if out[k + 1] is None else out[k + 1] - ck
        return out

    def axpy(a, x, y):
        out = []
        for k in range(max(len(x), len(y))):
            if k >= len(x):
                out.append(y[k])
            elif k >= len(y):
                out.append(a * x[k])
            else:
                out.append(y[k] + a * x[k])
        return out

    one = jnp.ones_like(nu[0])
    residual = [one]
    direction = [one]
    under = nu[0] - nu[1]
    step = nu[0] / under
    inverse = 1.0 / nu[0]
    step_inverse = under * inverse
    surface = [step]
    residual = axpy(-step, apply(direction), residual)
    for _ in range(2):
        gamma_next = form(residual, 0)
        delta = gamma_next - form(residual, 1)
        ratio = gamma_next * inverse
        under = delta - ratio * gamma_next * step_inverse
        step = gamma_next / under
        inverse = 1.0 / gamma_next
        step_inverse = under * inverse
        direction = axpy(ratio, direction, residual)
        surface = axpy(step, direction, surface)
        residual = axpy(-step, apply(direction), residual)
    return surface, residual


def kernel(
    lon_n, lat_n, lon_axis, lat_axis,
    thick_hbm, u_hbm, v_hbm, depth_hbm, mask_hbm, damp_hbm, eta_hbm,
    both_out,
    thick, u_buf, v_buf, depth_v, mask_v, damp_v, eta_v,
    send_east, recv_west, send_west, recv_east, send_lat, recv_lat,
    send_diag_east, recv_diag_west, send_diag_west, recv_diag_east, row_send, row_recv,
    load_sem, halo_send, halo_recv, all_send, all_recv,
):
    levels, rows, cols = u_hbm.shape
    n = lon_n * lat_n
    lon = lax.axis_index(lon_axis)
    lat = lax.axis_index(lat_axis)
    me = lon * lat_n + lat

    def peer(k):
        flat = lax.rem(me + k, n)
        return (flat // lat_n, lax.rem(flat, lat_n))

    def each_peer(f):
        if n <= 64:
            for k in sorted(range(1, n), key=lambda k: min(k, n - k)):
                f(k)
        else:
            lax.fori_loop(1, n, lambda k, c: (f(k), c)[1], 0)

    loads = []
    for k, (src, dst) in enumerate((
        (u_hbm, u_buf), (v_hbm, v_buf), (depth_hbm, depth_v), (mask_hbm, mask_v), (damp_hbm, damp_v), (eta_hbm, eta_v),
        (thick_hbm, thick)
    )):
        copy = pltpu.make_async_copy(src, dst, load_sem.at[k])
        loads.append(copy)
    for copy in loads[2:] + loads[:2]:
        copy.start()

    barrier = pltpu.get_barrier_semaphore()
    each_peer(lambda k: pl.semaphore_signal(barrier, inc=1, device_id=peer(k), device_id_type=MESH))

    def up(x, axis):
        return pltpu.roll(x, x.shape[axis] - 1, axis)

    def down(x, axis):
        return pltpu.roll(x, 1, axis)

    for copy in loads[2:]:
        copy.wait()
    wet_own = mask_v[...].astype(jnp.float32)
    damp_own = damp_v[...]
    deep_own = depth_v[...] * wet_own
    forced_own = wet_own * (damp_own * eta_v[...])
    row_own = lax.broadcasted_iota(jnp.int32, (rows, cols), 0)
    col_own = lax.broadcasted_iota(jnp.int32, (rows, cols), 1)
    inner_x = jnp.where(row_own < rows - 1, wet_own * up(wet_own, 0), 0.0)
    inner_y = jnp.where(col_own < cols - 1, wet_own * up(wet_own, 1), 0.0)
    tiles = cols // LANES
    for f, x in enumerate((deep_own, damp_own)):
        for c in range(tiles):
            span = slice(c * LANES, (c + 1) * LANES)
            send_west[f * tiles + c] = x[:HALO, span]
            send_east[f * tiles + c] = x[:, span]
        send_lat[0, f] = x[:, :LANES]
        send_lat[1, f] = x[:, cols - LANES:]
    scale = 1.0 / math.sqrt(levels)
    column = []
    for copy, buf in ((loads[0], u_buf), (loads[1], v_buf)):
        copy.wait()
        total = [None] * 4
        for k in range(levels):
            term = thick[k] * buf[k]
            total[k % 4] = term if total[k % 4] is None else total[k % 4] + term
        column.append(((total[0] + total[1]) + (total[2] + total[3])) * scale)
    east_own, north_own = column
    inner_x = inner_x * east_own
    inner_y = inner_y * north_own
    part_own = forced_own - (inner_x - down(inner_x, 0) + inner_y - down(inner_y, 1))
    last_east = jnp.broadcast_to(east_own[rows - 1:], (rows, cols))
    part_sent = jnp.where(row_own == 0, last_east, part_own)
    own = [deep_own, damp_own, part_own, east_own, north_own]
    lane_short = lax.broadcasted_iota(jnp.int32, (rows, LANES), 1)
    for c in range(tiles):
        span = slice(c * LANES, (c + 1) * LANES)
        send_west[2 * tiles + c] = part_own[:HALO, span]
        send_east[2 * tiles + c] = part_sent[:, span]
    north_last = north_own[:, cols - LANES:]
    send_west[3 * tiles] = north_last[:HALO]
    send_east[3 * tiles] = north_last

    def pack(fields, part):
        packed = None
        for f, x in enumerate(fields):
            edge = x[:, :LANES] if part == 0 else x[:, cols - LANES:]
            edge = edge if f == 0 else pltpu.roll(edge, HALO * f if part == 0 else LANES - HALO * f, 1)
            away = lane_short if part == 0 else LANES - 1 - lane_short
            packed = edge if packed is None else jnp.where(away >= HALO * f, edge, packed)
        return packed

    for part in (0, 1):
        send_diag_west[part] = pack((deep_own, damp_own, part_own, north_own), part)[:HALO]
        send_diag_east[part] = pack((deep_own, damp_own, part_sent, north_own), part)
    for f in range(2, FIELDS):
        send_lat[0, f] = own[f][:, :LANES]
        send_lat[1, f] = own[f][:, cols - LANES:]

    pl.semaphore_wait(barrier, n - 1)

    west = lax.rem(lon + lon_n - 1, lon_n)
    east = lax.rem(lon + 1, lon_n)

    def remote(src, dst, sem, target):
        return pltpu.make_async_remote_copy(
            src_ref=src, dst_ref=dst, send_sem=halo_send.at[sem], recv_sem=halo_recv.at[sem],
            device_id=target, device_id_type=MESH,
        )

    east_copy = remote(send_east, recv_west, 0, (east, lat))
    west_copy = remote(send_west, recv_east, 1, (west, lat))
    early, late = [], []
    for part in (0, 1):
        other = lat - 1 if part == 0 else lat + 1
        early.append([
            remote(send_diag_east.at[part], recv_diag_west.at[part], 2 + part, (east, other)),
            remote(send_lat.at[part], recv_lat.at[part], 4 + part, (lon, other)),
        ])
        late.append(remote(send_diag_west.at[part], recv_diag_east.at[part], 6 + part, (west, other)))
    has_south = lat > 0
    has_north = lat < lat_n - 1
    sends = (has_south, has_north)
    gets = (has_north, has_south)

    east_copy.start()
    for part in (0, 1):
        @pl.when(sends[part])
        def _():
            for copy in early[part]:
                copy.start()

    for part in (0, 1):
        @pl.when(jnp.logical_not(gets[part]))
        def _():
            recv_lat[part] = jnp.zeros((FIELDS, rows, LANES), jnp.float32)
            recv_diag_west[part] = jnp.zeros((rows, LANES), jnp.float32)
            recv_diag_east[part] = jnp.zeros((HALO, LANES), jnp.float32)

    for part in (0, 1):
        @pl.when(gets[part])
        def _():
            for copy in early[part]:
                copy.wait_recv()
    east_copy.wait_recv()

    north_side = lane_short < LANES // 2
    high, wide = 2 * rows, cols + LANES
    row_ext = lax.broadcasted_iota(jnp.int32, (high, wide), 0)
    col_ext = lax.broadcasted_iota(jnp.int32, (high, wide), 1)

    def side(f):
        return jnp.where(north_side, recv_lat[0, f], recv_lat[1, f])

    tops = [jnp.concatenate([own[f], side(f)], axis=1) for f in range(FIELDS)]

    west_copy.start()
    for part in (0, 1):
        @pl.when(sends[part])
        def _():
            late[part].start()

    def krylov(over, corners, last_row, at_x):
        def corner(f):
            north, south = corners
            if f > 0:
                north = pltpu.roll(north, LANES - HALO * f, 1)
                south = pltpu.roll(south, HALO * f, 1)
            return jnp.where(north_side, north, south)

        def extended(f):
            low = [over(f * tiles + c) for c in range(tiles)] + [corner(f)]
            return jnp.concatenate([tops[f], jnp.concatenate(low, axis=1)], axis=0)

        deep, damp, known = [extended(f) for f in range(3)]
        sum_east = jnp.concatenate([tops[3], jnp.broadcast_to(last_row, (rows, wide))], axis=0)
        low_north = jnp.concatenate([over(3 * tiles)] * tiles + [corner(3)], axis=1)
        sum_north = jnp.concatenate([tops[4], low_north], axis=0)
        wet = (deep > 0.0).astype(jnp.float32)
        damp = jnp.where(damp > 0.0, damp, 1.0)
        wet_x = wet * up(wet, 0)
        wet_y = wet * up(wet, 1)
        face_x = wet_x * 0.5 * (deep + up(deep, 0))
        face_y = wet_y * 0.5 * (deep + up(deep, 1))
        at_y = jnp.logical_or(col_ext == cols - 1, col_ext == wide - 1)
        flux_x = jnp.where(at_x, wet_x * sum_east, 0.0)
        flux_y = jnp.where(at_y, wet_y * sum_north, 0.0)
        rhs = known - (flux_x - down(flux_x, 0) + flux_y - down(flux_y, 1))
        face_w, face_s = down(face_x, 0), down(face_y, 1)
        inverse = 1.0 / (damp + face_x + face_w + face_y + face_s)

        def off(p):
            return face_x * up(p, 0) + face_w * down(p, 0) + face_y * up(p, 1) + face_s * down(p, 1)

        p0 = rhs * inverse
        w1 = off(p0)
        p1 = w1 * inverse
        w2 = off(p1)
        p2 = w2 * inverse
        return rhs, w1, w2, off(p2), p0, p1, p2

    corners_west = [recv_diag_west[part] for part in (0, 1)]
    row_of_west = jnp.concatenate(
        [recv_west[2 * tiles + c][:1] for c in range(tiles)]
        + [jnp.where(
            north_side,
            pltpu.roll(corners_west[0], LANES - 2 * HALO, 1),
            pltpu.roll(corners_west[1], 2 * HALO, 1),
        )[:1]],
        axis=1,
    )
    fields = krylov(lambda k: recv_west[k], corners_west, row_of_west, row_ext == high - 1)
    upper = row_own < HALO
    w0, w1, w2, w3, p0, p1, p2 = [jnp.where(upper, x[:rows, :cols], x[rows:, :cols]) for x in fields]

    lines = []
    for a, b in ((w0, p0), (w0, p1), (w1, p1), (w1, p2), (w2, p2), (w3, p2)):
        product = a * b
        folded = product[:, :LANES]
        for c in range(LANES, cols, LANES):
            folded = folded + product[:, c:c + LANES]
        lines.append(jnp.sum(folded, axis=0, keepdims=True))
    zero = jnp.zeros_like(lines[0])
    table = jnp.concatenate(lines + [zero] * (8 - len(lines)), axis=0)
    table = jnp.broadcast_to(jnp.sum(table, axis=1, keepdims=True), (8, LANES))
    pick = lax.broadcasted_iota(jnp.int32, (8, LANES), 1) == lax.broadcasted_iota(jnp.int32, (8, LANES), 0)
    row = jnp.sum(jnp.where(pick, table, 0.0), axis=0, keepdims=True)
    row_send[...] = row
    row_recv[me] = row

    def send_row(k):
        pltpu.make_async_remote_copy(
            src_ref=row_send, dst_ref=row_recv.at[me], send_sem=all_send, recv_sem=all_recv,
            device_id=peer(k), device_id_type=MESH,
        ).start()

    each_peer(send_row)

    for part in (0, 1):
        @pl.when(gets[part])
        def _():
            late[part].wait_recv()
    west_copy.wait_recv()

    corners = [
        jnp.concatenate([recv_diag_east[part], recv_diag_west[part][rows - HALO:]], axis=0) for part in (0, 1)
    ]
    fields = krylov(
        lambda k: jnp.concatenate([recv_east[k], recv_west[k][rows - HALO:]], axis=0),
        corners, row_of_west, jnp.logical_or(row_ext == rows - 1, row_ext == high - 1),
    )
    w0, w1, w2, w3, p0, p1, p2 = [x[:rows, :cols] for x in fields]

    east_copy.wait_send()
    west_copy.wait_send()
    for part in (0, 1):
        @pl.when(sends[part])
        def _():
            for copy in early[part]:
                copy.wait_send()
            late[part].wait_send()

    others = row_recv.at[pl.ds(0, n - 1)]
    pltpu.make_async_copy(others, others, all_recv).wait()
    if n <= 64:
        heap = [row_recv[k] for k in range(n)]
        while len(heap) > 1:
            heap = [a + b for a, b in zip(heap[::2], heap[1::2])] + heap[len(heap) - len(heap) % 2:]
        total = heap[0]
    else:
        total = jnp.sum(row_recv[...], axis=0)
    nu = [jnp.broadcast_to(total[:, k:k + 1], (ROWS, LANES)) for k in range(6)]
    s, r = scalars(nu)
    for c in range(0, cols, LANES):
        part = slice(c, c + LANES)
        both_out[0, :, part] = s[0] * p0[:, part] + s[1] * p1[:, part] + s[2] * p2[:, part]
        both_out[1, :, part] = (r[0] * w0[:, part] + r[1] * w1[:, part]) + (r[2] * w2[:, part] + r[3] * w3[:, part])
    pltpu.make_async_copy(others, others, all_send).wait()


def solution(mesh):
    lon_n, lat_n = mesh.shape["lon"], mesh.shape["lat"]
    n = lon_n * lat_n

    def body(u_vel, v_vel, thickness, depth, sea_mask, damping, eta_prev):
        levels, rows, cols = u_vel.shape
        f32 = jnp.float32
        hbm = pl.BlockSpec(memory_space=pl.ANY)
        vmem = pl.BlockSpec(memory_space=pltpu.VMEM)
        shape = pltpu.VMEM((2, rows, cols), f32)
        both = pl.pallas_call(
            functools.partial(kernel, lon_n, lat_n, "lon", "lat"),
            out_shape=shape,
            in_specs=[hbm] * 7,
            out_specs=vmem,
            scratch_shapes=[
                pltpu.SMEM((levels,), f32),
                pltpu.VMEM((levels, rows, cols), f32),
                pltpu.VMEM((levels, rows, cols), f32),
                pltpu.VMEM((rows, cols), f32),
                pltpu.VMEM((rows, cols), jnp.int32),
                pltpu.VMEM((rows, cols), f32),
                pltpu.VMEM((rows, cols), f32),
                pltpu.VMEM((3 * (cols // LANES) + 1, rows, LANES), f32),
                pltpu.VMEM((3 * (cols // LANES) + 1, rows, LANES), f32),
                pltpu.VMEM((3 * (cols // LANES) + 1, HALO, LANES), f32),
                pltpu.VMEM((3 * (cols // LANES) + 1, HALO, LANES), f32),
                pltpu.VMEM((2, FIELDS, rows, LANES), f32),
                pltpu.VMEM((2, FIELDS, rows, LANES), f32),
                pltpu.VMEM((2, rows, LANES), f32),
                pltpu.VMEM((2, rows, LANES), f32),
                pltpu.VMEM((2, HALO, LANES), f32),
                pltpu.VMEM((2, HALO, LANES), f32),
                pltpu.VMEM((1, LANES), f32),
                pltpu.VMEM((n, 1, LANES), f32),
                pltpu.SemaphoreType.DMA((7,)),
                pltpu.SemaphoreType.DMA((8,)),
                pltpu.SemaphoreType.DMA((8,)),
                pltpu.SemaphoreType.DMA,
                pltpu.SemaphoreType.DMA,
            ],
            compiler_params=pltpu.CompilerParams(collective_id=0, has_side_effects=True),
        )(thickness, u_vel, v_vel, depth, sea_mask, damping, eta_prev)
        return both[0], both[1]


    placed = P("lon", "lat")
    return jax.shard_map(
        body,
        mesh=mesh,
        in_specs=(P(None, "lon", "lat"), P(None, "lon", "lat"), P(), placed, placed, placed, placed),
        out_specs=(placed, placed),
        check_vma=False,
    )
```
